128 devices in a mesh: obs: 8 (over y, core), src: 16 (over x, z).
Axes of the slice: x: 4, y: 4, z: 4, core: 2. Of those that a mesh axis runs over, the one named last changes fastest.
Arguments:
- data: float32 [1024, 1536], P(('obs', 'src')), may hold values from -170 to 170
- obs_points: float32 [1024, 3, 256], P('obs'), may hold values from 0 to 32, as said below
- src_points: float32 [1024, 3, 256], P('src'), may hold values from -0.4 to 32, as said below
- obs_basis: float32 [1024, 64, 1536], P(('obs', 'src')), may hold values from -0.09375 to 0.09375
- src_basis: float32 [1024, 64, 256], P(('src', 'obs')), may hold values from -0.375 to 0.375
- couplings: float32 [8, 16, 320, 64, 64], P('obs', 'src'), may hold values from -0.75 to 0.75
- near_pairs: int32 [8, 16, 72], P('obs', 'src'), may hold values from -1 to 8191, as said below
- far_pairs: int32 [8, 16, 320], P('obs', 'src'), may hold values from -1 to 8191, as said below
Outputs:
- sources: float32 [1024, 256], P(('src', 'obs'))
- residual: float32 [1024, 1536], P(('obs', 'src'))
- normal_residual: float32 [1024, 256], P(('src', 'obs'))
- misfit: float32 [3], replicated
The draws below stay inside these ranges and needn't reach their ends.
Inputs may be any that keep to these rules, and one draw needn't show every extreme that they name: Live entries of every block come first and -1 fills the remaining slots; a live entry o * 64 + s pairs local observation leaf o with local source leaf s; no pair is listed twice, and no pair is in both near_pairs and far_pairs. Leaves lie on surface tiles: observation leaf n on tile row (n // 32 + c) % 32, tile column n % 32, with one c of 0 to 3 for all leaves of a draw; source leaf m = j * 64 + h * 8 + l (0 <= h < 8, 0 <= l < 8) on tile row (l % 4) * 8 + h, tile column j * 2 + l // 4. A near pair joins two leaves whose tile rows differ by at most one and whose tile columns differ by at most one. `far_pairs`: live entries of every block come first and -1 fills the remaining slots; a live entry o * 64 + s pairs local observation leaf o with local source leaf s, coupled by the matrix in the same slot of couplings; no pair is listed twice; on the tiles described for near_pairs, the larger of its two leaves' tile row and tile column differences is two or three. `obs_points`: the third coordinate of every observation point lies in [0.5, 0.9]. `src_points`: the third coordinate of every source lies in [-0.4, -0.1].
All inputs are finite; a program needn't handle non-finite values.
Results may differ from the reference program's by a relative error of at most 0.0003.
Values sent between devices are 32-bit elements; how exact they have to be, the bound alone decides.
No kernel may reach another device: no remote copies, remote signals or barrier semaphores. Data moves between devices by JAX's collectives and lax.ppermute only.
A program may use at most 128 MiB of HBM per device.

```python
import jax
import jax.numpy as jnp
from jax import lax

LEAF = 256
RANK = 64
LEAF_DEV = 8
ITERS = 2
TILE_COLS = 32
TILE_ROWS = 32
OBS_SUB = 128
SRC_SUB = 64
OBS_LEAVES = 1024
SRC_LEAVES = 1024
NEAR_CAP = 72
FAR_CAP = 320
N_OBS = 8
N_SRC = 16


def tile_shift(key):
    return jax.random.randint(jax.random.fold_in(key, 11), (), 0, 4)


def obs_tiles(key):
    leaves = jnp.arange(OBS_LEAVES, dtype=jnp.int32)
    row_index = (leaves // TILE_COLS + tile_shift(key)) % TILE_ROWS
    return (row_index, leaves % TILE_COLS)


def src_tiles():
    leaves = jnp.arange(SRC_LEAVES, dtype=jnp.int32)
    subtree = leaves // SRC_SUB
    within = leaves % SRC_SUB
    holder = within // LEAF_DEV
    slot_index = within % LEAF_DEV
    row_index = slot_index % 4 * N_OBS + holder
    col_index = subtree * (LEAF_DEV // 4) + slot_index // 4
    return (row_index, col_index)


def pair_table(key, salt_value, nearest, farthest, keep_of, capacity):
    obs_row, obs_col = obs_tiles(key)
    src_row, src_col = src_tiles()
    obs_row = obs_row.reshape(N_OBS, 1, OBS_SUB, 1)
    obs_col = obs_col.reshape(N_OBS, 1, OBS_SUB, 1)
    src_row = src_row.reshape(1, N_SRC, 1, SRC_SUB)
    src_col = src_col.reshape(1, N_SRC, 1, SRC_SUB)
    row_gap = obs_row - src_row
    distance = jnp.maximum(jnp.abs(row_gap), jnp.abs(obs_col - src_col))
    candidate = (distance >= nearest) & (distance <= farthest)
    salted = jax.random.fold_in(key, salt_value)
    coin_draw = jax.random.randint(jax.random.fold_in(salted, 1), candidate.shape, 0, keep_of)
    chosen = candidate & ((row_gap == 0) | (coin_draw == 0))
    span_width = OBS_SUB * SRC_SUB
    chosen = chosen.reshape(N_OBS * N_SRC, span_width)
    block_keys = jax.random.split(jax.random.fold_in(salted, 2), N_OBS * N_SRC)
    orders = jax.vmap(lambda block_key: jax.random.permutation(block_key, span_width))(block_keys)
    scores = jnp.where(chosen, 0, span_width) + orders
    ranked = jnp.argsort(scores, axis=1, stable=True)[:, :capacity].astype(jnp.int32)
    is_live = jnp.take_along_axis(chosen, ranked, axis=1)
    listing = jnp.where(is_live, ranked, -1)
    return listing.reshape(N_OBS, N_SRC, capacity).astype(jnp.int32)


def draw_near_pairs(key, part):
    return pair_table(key, 21, 0, 1, 4, NEAR_CAP)


def draw_far_pairs(key, part):
    return pair_table(key, 37, 2, 3, 2, FAR_CAP)


def draw_obs_points(key, part):
    row_index, col_index = obs_tiles(key)
    spread = jax.random.uniform(jax.random.fold_in(key, 3), (OBS_LEAVES, 3, LEAF), dtype=jnp.float32)
    east = col_index[:, None].astype(jnp.float32) + spread[:, 0]
    north = row_index[:, None].astype(jnp.float32) + spread[:, 1]
    height = 0.5 + 0.4 * spread[:, 2]
    return jnp.stack([east, north, height], axis=1)


def draw_src_points(key, part):
    row_index, col_index = src_tiles()
    spread = jax.random.uniform(jax.random.fold_in(key, 4), (SRC_LEAVES, 3, LEAF), dtype=jnp.float32)
    east = col_index[:, None].astype(jnp.float32) + spread[:, 0]
    north = row_index[:, None].astype(jnp.float32) + spread[:, 1]
    depth = -0.4 + 0.3 * spread[:, 2]
    return jnp.stack([east, north, depth], axis=1)


def draw_data(key, part):
    noise = jnp.clip(jax.random.normal(jax.random.fold_in(key, 5), (OBS_LEAVES, 6 * LEAF), dtype=jnp.float32), -4.0, 4.0)
    leaves = jnp.arange(OBS_LEAVES, dtype=jnp.float32) / OBS_LEAVES
    rough = jnp.exp(jax.random.uniform(jax.random.fold_in(key, 6), (OBS_LEAVES, 1), dtype=jnp.float32, maxval=1.19))
    rising = jnp.exp(1.0986 * leaves)[:, None]
    return noise * rough * rising


def level_of(key, extent, pieces, smallest, largest):
    factor_of, own = 1.0, jax.random.fold_in(key, 6)
    for axis_at, shards_of in pieces:
        heights = jnp.exp(jax.random.uniform(jax.random.fold_in(own, axis_at), (shards_of,), jnp.float32, smallest / len(pieces), largest / len(pieces)))
        factor_of = factor_of * jnp.repeat(heights, extent[axis_at] // shards_of).reshape([-1 if axis == axis_at else 1 for axis in range(len(extent))])
    return factor_of


def scatter_about(own_key, shape, scale, limit, pieces=(), kind=jnp.bfloat16):
    result = jax.random.normal(own_key, shape, jnp.float32) * scale
    if len(pieces) > 0:
        result = level_of(own_key, shape, pieces, -0.22, 0.18) * result
    return jnp.clip(result, min=-limit, max=limit).astype(kind)


def setup_inputs(seed: int = 0) -> dict:
    key_list = jax.random.split(jax.random.key(seed), 9)
    return {
        "data": draw_data(jax.random.fold_in(key_list[8], 71), 0),
        "obs_points": draw_obs_points(jax.random.fold_in(key_list[8], 71), 0),
        "src_points": draw_src_points(jax.random.fold_in(key_list[8], 71), 0),
        "obs_basis": scatter_about(key_list[3], (OBS_LEAVES, RANK, 6 * LEAF), (64 * RANK) ** -0.5, 0.09375, ((0, 128),), jnp.float32),
        "src_basis": scatter_about(key_list[4], (SRC_LEAVES, RANK, LEAF), LEAF ** -0.5, 0.375, ((0, 128),), jnp.float32),
        "couplings": scatter_about(key_list[5], (N_OBS, N_SRC, FAR_CAP, RANK, RANK), RANK ** -0.5, 0.75, ((0, 8), (1, 16)), jnp.float32),
        "near_pairs": draw_near_pairs(jax.random.fold_in(key_list[8], 71), 0),
        "far_pairs": draw_far_pairs(jax.random.fold_in(key_list[8], 71), 0),
    }


exact = lax.Precision.HIGHEST
pair_group = 8

def tensor_parts(obs_pts, src_pts):
    diff_x = obs_pts[:, 0, :, None] - src_pts[:, 0, None, :]
    diff_y = obs_pts[:, 1, :, None] - src_pts[:, 1, None, :]
    diff_z = obs_pts[:, 2, :, None] - src_pts[:, 2, None, :]
    inverse = lax.rsqrt(diff_x * diff_x + diff_y * diff_y + diff_z * diff_z)
    inv_cube = inverse * inverse * inverse / obs_pts.shape[-1]
    inv_fifth = 3.0 * inv_cube * inverse * inverse
    return (inv_fifth * diff_x * diff_x - inv_cube, inv_fifth * diff_x * diff_y, inv_fifth * diff_x * diff_z, inv_fifth * diff_y * diff_y - inv_cube, inv_fifth * diff_y * diff_z, inv_fifth * diff_z * diff_z - inv_cube)

def near_loop(obs_ids, src_ids, pair_count, obs_pts, src_pts, source, target, forward, group_size):
    length = obs_ids.shape[0]
    padding = -length % group_size
    obs_ids = jnp.concatenate([obs_ids.astype(jnp.int32), jnp.zeros((padding,), jnp.int32)])
    src_ids = jnp.concatenate([src_ids.astype(jnp.int32), jnp.zeros((padding,), jnp.int32)])

    def one_group(group_index, running):
        first_slot = (group_index * group_size).astype(jnp.int32)
        obs_take = lax.dynamic_slice_in_dim(obs_ids, first_slot, group_size)
        src_take = lax.dynamic_slice_in_dim(src_ids, first_slot, group_size)
        in_range = first_slot + jnp.arange(group_size, dtype=jnp.int32) < pair_count
        tensor = tensor_parts(obs_pts[obs_take], src_pts[src_take])
        if forward:
            strengths = jnp.where(in_range[:, None], source[src_take], 0.0)[:, None, :]
            contributions = jnp.stack([lax.optimization_barrier(jnp.sum(component * strengths, axis=2)) for component in tensor], axis=1)
            return running.at[obs_take].add(contributions.reshape(group_size, -1))
        residual_rows = jnp.where(in_range[:, None], source[obs_take], 0.0).reshape(group_size, 6, -1)
        weighted = tensor[0] * residual_rows[:, 0, :, None]
        for which in range(1, 6):
            weighted = weighted + tensor[which] * residual_rows[:, which, :, None]
        return running.at[src_take].add(lax.optimization_barrier(jnp.sum(weighted, axis=1)))
    groups = ((pair_count + group_size - 1) // group_size).astype(jnp.int32)
    return lax.fori_loop(0, groups, one_group, target)

def compact(chosen):
    length = chosen.shape[0]
    position = (jnp.cumsum(chosen.astype(jnp.int32)) - 1).astype(jnp.int32)
    target = jnp.where(chosen, position, length)
    picked = jnp.zeros((length,), jnp.int32).at[target].set(jnp.arange(length, dtype=jnp.int32), mode='drop')
    return (picked, jnp.sum(chosen.astype(jnp.int32)).astype(jnp.int32))

def decode(pairs, capacity):
    flat = pairs.reshape(-1)
    slots = jnp.arange(flat.shape[0], dtype=jnp.int32)
    block_id = slots // capacity
    live_slot = flat >= 0
    safe_value = jnp.where(live_slot, flat, 0)
    obs_ids = (block_id // N_SRC * OBS_SUB + safe_value // SRC_SUB).astype(jnp.int32)
    src_ids = (block_id % N_SRC * SRC_SUB + safe_value % SRC_SUB).astype(jnp.int32)
    return (live_slot, obs_ids, src_ids)

def reference(data, obs_points, src_points, obs_basis, src_basis, couplings, near_pairs, far_pairs):
    near_live, near_obs, near_src = decode(near_pairs, NEAR_CAP)
    picked, near_count = compact(near_live)
    near_obs = near_obs[picked]
    near_src = near_src[picked]
    far_live, far_obs, far_src = decode(far_pairs, FAR_CAP)
    blocks_flat = couplings.reshape(-1, RANK, RANK)

    def forward(direction):
        coeffs = jnp.einsum('nkq,nq->nk', src_basis, direction, precision=exact)
        chosen_coeffs = jnp.where(far_live[:, None], coeffs[far_src], 0.0)
        far_terms = jnp.einsum('ckl,cl->ck', blocks_flat, chosen_coeffs, precision=exact)
        obs_coeffs = jnp.zeros((OBS_LEAVES, RANK), jnp.float32).at[far_obs].add(far_terms)
        far_part = jnp.einsum('nk,nkm->nm', obs_coeffs, obs_basis, precision=exact)
        near_part = near_loop(near_obs, near_src, near_count, obs_points, src_points, direction, jnp.zeros((OBS_LEAVES, 6 * LEAF), jnp.float32), True, pair_group)
        return far_part + near_part

    def adjoint(values):
        coeffs = jnp.einsum('nkm,nm->nk', obs_basis, values, precision=exact)
        chosen_coeffs = jnp.where(far_live[:, None], coeffs[far_obs], 0.0)
        far_terms = jnp.einsum('ckl,ck->cl', blocks_flat, chosen_coeffs, precision=exact)
        src_coeffs = jnp.zeros((SRC_LEAVES, RANK), jnp.float32).at[far_src].add(far_terms)
        far_part = jnp.einsum('nk,nkq->nq', src_coeffs, src_basis, precision=exact)
        near_part = near_loop(near_obs, near_src, near_count, obs_points, src_points, values, jnp.zeros((SRC_LEAVES, LEAF), jnp.float32), False, pair_group)
        return far_part + near_part
    residual = data
    normal = adjoint(residual)
    gamma_now = jnp.sum(normal * normal)
    history = [jnp.sum(residual * residual)]
    direction = normal
    solution = jnp.zeros_like(normal)
    for iteration in range(ITERS):
        projected = forward(direction)
        step_size = gamma_now / jnp.sum(projected * projected)
        solution = solution + step_size * direction
        residual = residual - step_size * projected
        history.append(jnp.sum(residual * residual))
        normal = adjoint(residual)
        gamma_next = jnp.sum(normal * normal)
        direction = normal + gamma_next / gamma_now * direction
        gamma_now = gamma_next
    return (solution, residual, normal, jnp.stack(history))
```

```python
import functools

import jax
import jax.numpy as jnp
from jax import lax
from jax.experimental import pallas as pl
from jax.experimental.pallas import tpu as pltpu
from jax.sharding import Mesh
from jax.sharding import PartitionSpec as P

OBS_SRC = ("obs_0", "obs_1", "src_0", "src_1")
SRC = ("src_0", "src_1")
OBS = ("obs_0", "obs_1")
SRC_OBS = ("src_0", "src_1", "obs_0", "obs_1")

F32 = jnp.float32
BF16 = jnp.bfloat16
PAIRS = 72
ROWS = 16
MIB = 1 << 20


def split(value):
    high = value.astype(BF16)
    return high, (value - high.astype(F32)).astype(BF16)


def mm(a, b):
    return lax.dot_general(a, b, (((1,), (0,)), ((), ())), preferred_element_type=F32)


def mm_nt(a, b):
    return lax.dot_general(a, b, (((1,), (1,)), ((), ())), preferred_element_type=F32)


def iota(shape, dim):
    return lax.broadcasted_iota(jnp.int32, shape, dim)


def lane_scalar(block, which):
    lanes = iota(block.shape, 1)
    return jnp.sum(jnp.where(lanes == 64 + which, block, 0.0), axis=1, keepdims=True)


def total(value):
    return jnp.sum(jnp.sum(value, axis=1, keepdims=True), axis=0, keepdims=True)


def with_scalars(block, scalars):
    lanes = iota(block.shape, 1)
    for which, value in enumerate(scalars):
        block = jnp.where(lanes == 64 + which, value, block)
    return block


def setup_near(slots, column, near_row, far_row, obs, src, kh, kl, pq, count, oo, oot, ost, os, fo, fot, fs, fst):
    j = column[0]
    f = near_row[...]
    live = f >= 0
    o = lax.shift_right_arithmetic(f, 6)
    s = jnp.where(live, f & 63, -1)
    oc = jnp.where(live, lax.shift_right_arithmetic(o, 5) * 4 + (o & 31) - (2 * j - 1), -1)
    a = (iota((16, 128), 0) == oc).astype(F32)
    oot[...] = a.astype(BF16)
    oo[...] = a.T.astype(BF16)
    a = (iota((64, 128), 0) == s).astype(F32)
    ost[...] = a.astype(BF16)
    os[...] = a.T.astype(BF16)
    f = far_row[...]
    live = f >= 0
    o = jnp.where(live, lax.shift_right_arithmetic(f, 6), -1)
    s = jnp.where(live, f & 63, -1)
    a = (iota((128, 384), 0) == o).astype(F32)
    fot[...] = a.astype(BF16)
    fo[...] = a.T.astype(BF16)
    a = (iota((64, 384), 0) == s).astype(F32)
    fst[...] = a.astype(BF16)
    fs[...] = a.T.astype(BF16)
    pq[...] = jnp.zeros_like(pq)

    n = lax.fori_loop(0, PAIRS, lambda t, c: c + jnp.where(slots[t] >= 0, 1, 0), 0)
    count[0] = n

    def one(t, carry):
        name = slots[t]
        p = obs[lax.shift_right_arithmetic(name, 6)]
        q = src[name & 63]
        centre = 0.5 * (jnp.mean(p, axis=1, keepdims=True) + jnp.mean(q, axis=1, keepdims=True))
        p = p - centre
        q = q - centre
        for c in range(3):
            pq[c, pl.ds(t, 1), :] = p[c : c + 1]
            pq[3 + c, pl.ds(t, 1), :] = q[c : c + 1]
        pt = jnp.concatenate([p, jnp.zeros((5, 256), F32)], axis=0).T
        for r in range(0, 256, 32):
            dx = pt[r : r + 32, 0:1] - q[0:1]
            dy = pt[r : r + 32, 1:2] - q[1:2]
            dz = pt[r : r + 32, 2:3] - q[2:3]
            inverse = lax.rsqrt(dx * dx + dy * dy + dz * dz)
            square = inverse * inverse
            fifth = square * square * (inverse * (1.0 / 256.0))
            high, low = split(fifth)
            kh[t, r : r + 32, :] = high
            kl[t, r : r + 32, :] = low
        return carry

    lax.fori_loop(0, n, one, 0)


def setup_far(c, wh, wl):
    for g in range(4):
        high, low = split(jnp.concatenate([c[4 * g + n] for n in range(4)], axis=1))
        wh[0, 64 * g : 64 * g + 64, :] = high
        wl[0, 64 * g : 64 * g + 64, :] = low


def far_matrices(x, pick, place, wh, wl, forward):
    half = jnp.where(iota(x.shape, 1) < 64, x, 0.0)
    half = half + pltpu.roll(half, 64, 1)
    high, low = split(jnp.concatenate([half, half], axis=1))
    lanes = lax.shift_right_logical(iota((16, 256), 1), 6)
    slot = iota((16, 256), 0)
    row_group = lanes == lax.shift_right_logical(slot, 2)
    col_group = lanes == (slot & 3)
    enter, leave = (col_group, row_group) if forward else (row_group, col_group)
    multiply = mm_nt if forward else mm
    picked_high = mm(pick, high)
    picked_low = mm(pick, low)
    terms = []
    for t in range(20):
        at = slice(16 * t, 16 * t + 16)
        h = jnp.where(enter, picked_high[at], 0.0).astype(BF16)
        l = jnp.where(enter, picked_low[at], 0.0).astype(BF16)
        both = multiply(jnp.concatenate([h, l], axis=0), wh[t])
        terms.append(jnp.where(leave, both[:16] + both[16:] + multiply(h, wl[t]), 0.0))
    high, low = split(jnp.concatenate(terms, axis=0))
    out = mm(place, high) + mm(place, low)
    out = out[:, :128] + out[:, 128:]
    return out + pltpu.roll(out, 64, 1)


def near_products(n, moments, results, kh, kl, multiply):
    def four(g, carry):
        for b in range(4):
            t = 4 * g + b
            at = pl.ds(pl.multiple_of(t * ROWS, ROWS), ROWS)
            high, low = split(jnp.concatenate([moments[0, at, :], moments[1, at, :]], axis=1))
            both = multiply(jnp.concatenate([high, low], axis=0), kh[t])
            both = both[:ROWS] + both[ROWS:] + multiply(high, kl[t])
            results[0, at, :] = both[:, :128]
            results[1, at, :] = both[:, 128:]
        return carry

    lax.fori_loop(0, lax.shift_right_logical(n + 3, 2), four, 0)


def store_moment(moments, g, c, value):
    at = pl.ds(g * (8 * ROWS) + c, 8, ROWS)
    moments.at[0][at, :] = value[:, :128]
    moments.at[1][at, :] = value[:, 128:]


def load_result(results, g, c):
    at = pl.ds(g * (8 * ROWS) + c, 8, ROWS)
    return jnp.concatenate([results.at[0][at, :], results.at[1][at, :]], axis=1)


def adjoint_block(count, column, recv, kh, kl, pq, oo, ost, fo, fst, wh, wl, out, yb, yp, moments, results, values):
    n = count[0]
    j = column[0]
    for t in range(4):
        col = 2 * j - 1 + t
        inside = jnp.logical_and(col >= 0, col < 32)
        holder = lax.shift_right_logical(jnp.clip(col, 0, 31), 3)
        for row in range(4):
            for half in range(2):
                piece = recv[row * 4 + holder, 2 * t + half : 2 * t + half + 1, 0:768]
                if t in (0, 3):
                    piece = jnp.where(inside, piece, 0.0)
                yb[4 * row + t : 4 * row + t + 1, 768 * half : 768 * half + 768] = piece
    high, low = split(yb[...])
    yp[...] = mm(oo[0:80, :], high) + mm(oo[0:80, :], low)
    values[...] = jnp.zeros_like(values)
    groups = lax.shift_right_logical(n + 7, 3)

    def enter(g, carry):
        at = pl.ds(pl.multiple_of(g * 8, 8), 8)
        y = [yp[at, 256 * a : 256 * a + 256] for a in range(6)]
        px, py, pz = (pq[c, at, :] for c in range(3))
        trace = y[0] + y[3] + y[5]
        hxx, hyy, hzz = (3.0 * y[a] - trace for a in (0, 3, 5))
        hxy, hxz, hyz = (3.0 * y[a] for a in (1, 2, 4))
        ax, ay, az = hxx * px, hyy * py, hzz * pz
        bx, by, bz = hxy * py + hxz * pz, hxy * px + hyz * pz, hxz * px + hyz * py
        constant = px * (ax + hxy * py) + py * (ay + hyz * pz) + pz * (az + hxz * px)
        rows = (constant, 2.0 * ax + bx, 2.0 * ay + by, 2.0 * az + bz, hxx, hxy, hxz, hyy, hyz, hzz)
        for c, row in enumerate(rows):
            store_moment(moments, g, c, row)
        return carry

    lax.fori_loop(0, groups, enter, 0)
    near_products(n, moments, results, kh, kl, mm)

    def leave(g, carry):
        at = pl.ds(pl.multiple_of(g * 8, 8), 8)
        w = [load_result(results, g, c) for c in range(10)]
        qx, qy, qz = (pq[3 + c, at, :] for c in range(3))
        z = w[0] + qx * (w[4] * qx + w[5] * qy - w[1]) + qy * (w[7] * qy + w[8] * qz - w[2])
        z = z + qz * (w[9] * qz + w[6] * qx - w[3])
        values[at, :] = jnp.where(iota((8, 256), 0) + g * 8 < n, z, 0.0)
        return carry

    lax.fori_loop(0, groups, leave, 0)
    high, low = split(values[...])
    out[:, 0:256] = mm(ost[...], high) + mm(ost[...], low)
    tails = [recv[k, :, 768:896] for k in range(16)]
    coeffs = far_matrices(jnp.concatenate(tails, axis=0), fo[0:320, :], fst[:, 0:320], wh, wl, False)
    sums = functools.reduce(jnp.add, tails)
    for k in range(8):
        part = coeffs[8 * k : 8 * k + 8]
        out[8 * k : 8 * k + 8, 256:384] = jnp.where(iota((8, 128), 1) < 64, part, sums)


def forward_block(count, column, recv, kh, kl, pq, os, oot, fs, fot, wh, wl, out, xp, moments, results, values, yb):
    n = count[0]
    j = column[0]
    high, low = split(recv[:, 0:256])
    xp[...] = mm(os[0:80, :], high) + mm(os[0:80, :], low)
    values[...] = jnp.zeros_like(values)
    groups = lax.shift_right_logical(n + 7, 3)

    def enter(g, carry):
        at = pl.ds(pl.multiple_of(g * 8, 8), 8)
        x = xp[at, :]
        qx, qy, qz = (pq[3 + c, at, :] for c in range(3))
        x1, x2, x3 = x * qx, x * qy, x * qz
        rows = (x, x1, x2, x3, x1 * qx, x1 * qy, x1 * qz, x2 * qy, x2 * qz, x3 * qz)
        for c, row in enumerate(rows):
            store_moment(moments, g, c, row)
        return carry

    lax.fori_loop(0, groups, enter, 0)
    near_products(n, moments, results, kh, kl, mm_nt)

    def leave(g, carry):
        at = pl.ds(pl.multiple_of(g * 8, 8), 8)
        s = [load_result(results, g, c) for c in range(10)]
        px, py, pz = (pq[c, at, :] for c in range(3))
        ax, ay, az = px * s[0] - s[1], py * s[0] - s[2], pz * s[0] - s[3]
        xx = px * (ax - s[1]) + s[4]
        xy = py * ax - px * s[2] + s[5]
        xz = pz * ax - px * s[3] + s[6]
        yy = py * (ay - s[2]) + s[7]
        yz = pz * ay - py * s[3] + s[8]
        zz = pz * (az - s[3]) + s[9]
        trace = xx + yy + zz
        inside = iota((8, 256), 0) + g * 8 < n
        parts = (3.0 * xx - trace, 3.0 * xy, 3.0 * xz, 3.0 * yy - trace, 3.0 * yz, 3.0 * zz - trace)
        for a, part in enumerate(parts):
            values[at, 256 * a : 256 * a + 256] = jnp.where(inside, part, 0.0)
        return carry

    lax.fori_loop(0, groups, leave, 0)
    high, low = split(values[...])
    yb[...] = mm(oot[...], high) + mm(oot[...], low)
    for t in range(4):
        holder = lax.shift_right_logical(jnp.clip(2 * j - 1 + t, 0, 31), 3)
        for row in range(4):
            for half in range(2):
                piece = yb[4 * row + t : 4 * row + t + 1, 768 * half : 768 * half + 768]
                out[row * 4 + holder, 2 * t + half : 2 * t + half + 1, 0:768] = piece
    tails = [recv[8 * k : 8 * k + 8, 256:384] for k in range(8)]
    coeffs = far_matrices(recv[:, 256:384], fs[0:320, :], fot[:, 0:320], wh, wl, True)
    sums = functools.reduce(jnp.add, tails)
    for k in range(16):
        out[k, :, 768:896] = jnp.where(iota((8, 128), 1) < 64, coeffs[8 * k : 8 * k + 8], sums)


def send_residual(zone, values, basis, out, scalars):
    lanes = iota((64, 128), 1)
    columns = jnp.zeros((64, 128), F32)
    for r in range(8):
        column = jnp.sum(basis[r] * values[r : r + 1, :], axis=1, keepdims=True)
        columns = jnp.where(lanes == r, column, columns)
    columns = jnp.concatenate([columns, jnp.zeros((64, 128), F32)], axis=0)
    tail = with_scalars(columns.T[0:8, :], scalars)
    for k in range(16):
        out[k, :, 768:896] = tail

    def rows(d):
        for t in range(4):
            r = 2 * d - 1 + t
            if 0 <= r < 8:
                for half in range(2):
                    piece = values[r : r + 1, 768 * half : 768 * half + 768]
                    out[4 * zone + d, 2 * t + half : 2 * t + half + 1, 0:768] = piece

    for d in range(4):
        rows(d)

    @pl.when(zone > 0)
    def _():
        rows(-1)

    @pl.when(zone < 3)
    def _():
        rows(4)


def start_obs(zone, data, basis, out):
    send_residual(zone[0], data, basis, out, (total(data[...] * data[...]),))


def gather_projected(zone, recv, basis, p):
    tail = functools.reduce(jnp.add, [recv[k, :, 768:896] for k in range(16)])
    columns = jnp.where(iota((8, 128), 1) < 64, tail, 0.0).T
    for r in range(8):
        far = jnp.sum(basis[r] * columns[0:64, r : r + 1], axis=0, keepdims=True)
        for half in range(2):
            value = far[:, 768 * half : 768 * half + 768]
            for t in range(4):
                if (r + 1 - t) % 2 == 0:
                    d = (r + 1 - t) // 2
                    piece = recv[jnp.clip(4 * zone + d, 0, 15), 2 * t + half : 2 * t + half + 1, 0:768]
                    if d == -1:
                        piece = jnp.where(zone > 0, piece, 0.0)
                    if d == 4:
                        piece = jnp.where(zone < 3, piece, 0.0)
                    value = value + piece
            p[r : r + 1, 768 * half : 768 * half + 768] = value
    return tail


def first_obs(zone, recv, data, basis, p, gammas, out):
    z = zone[0]
    gammas[...] = gather_projected(z, recv, basis, p)
    pv, dv = p[...], data[...]
    send_residual(z, p, basis, out, (total(pv * pv), total(dv * pv)))


def second_obs(zone, recv, data, p0, gamma0, sums1, basis, p, r, gammas, out):
    z = zone[0]
    tail = gather_projected(z, recv, basis, p)
    gammas[...] = tail
    g0 = lane_scalar(gamma0[...], 0)
    pv = p[...] + (lane_scalar(tail, 0) / g0) * p0[...]
    rv = data[...] - (g0 / lane_scalar(sums1[...], 0)) * p0[...]
    p[...] = pv
    r[...] = rv
    send_residual(z, p, basis, out, (total(pv * pv), total(rv * pv)))


def gather_normal(recv, basis, q):
    block = functools.reduce(jnp.add, [recv[k] for k in range(8)])
    tail = block[:, 256:384]
    columns = jnp.where(iota((8, 128), 1) < 64, tail, 0.0).T
    for r in range(8):
        far = jnp.sum(basis[r] * columns[0:64, r : r + 1], axis=0, keepdims=True)
        q[r : r + 1, :] = block[r : r + 1, 0:256] + far
    return tail


def send_direction(x, basis, out):
    lanes = iota((64, 128), 1)
    columns = jnp.zeros((64, 128), F32)
    for r in range(8):
        column = jnp.sum(basis[r] * x[r : r + 1], axis=1, keepdims=True)
        columns = jnp.where(lanes == r, column, columns)
    columns = jnp.concatenate([columns, jnp.zeros((64, 128), F32)], axis=0)
    tail = with_scalars(columns.T[0:8, :], (total(x * x),))
    for k in range(8):
        out[k, :, 0:256] = x
        out[k, :, 256:384] = tail


def first_src(recv, basis, n0, sums, out):
    sums[...] = gather_normal(recv, basis, n0)
    send_direction(n0[...], basis, out)


def second_src(recv, basis, n0, gamma0, n1, sums, out):
    tail = gather_normal(recv, basis, n1)
    sums[...] = tail
    x = n0[...] - (lane_scalar(gamma0[...], 0) / lane_scalar(tail, 0)) * n1[...]
    n1[...] = x
    send_direction(x, basis, out)


def last_src(recv, basis, n0, n1, gamma0, gamma1, sums0, sums1, r1, p1, found, residual, normal, misfit):
    tail = gather_normal(recv, basis, normal)
    g0, g1 = lane_scalar(gamma0[...], 0), lane_scalar(gamma1[...], 0)
    s1 = sums1[...]
    curve0, cross0 = lane_scalar(s1, 0), lane_scalar(s1, 1)
    curve1, cross1 = lane_scalar(tail, 0), lane_scalar(tail, 1)
    step0, step1 = g0 / curve0, g1 / curve1
    normal[...] = n1[...] - step1 * normal[...]
    found[...] = step0 * n0[...] + step1 * (n1[...] + (g1 / g0) * n0[...])
    residual[...] = r1[...] - step1 * p1[...]
    m0 = lane_scalar(sums0[...], 0)
    m1 = m0 - 2.0 * step0 * cross0 + step0 * step0 * curve0
    m2 = m1 - 2.0 * step1 * cross1 + step1 * step1 * curve1
    lanes = iota((8, 128), 1)
    misfit[...] = jnp.where(lanes == 0, m0, jnp.where(lanes == 1, m1, m2))


VM = pl.BlockSpec(memory_space=pltpu.VMEM)
SM = pl.BlockSpec(memory_space=pltpu.SMEM)


def shape(*dims, dtype=F32):
    return jax.ShapeDtypeStruct(dims, dtype)


def call(kernel, outs, ins, scratch=(), out_specs=None, scalars=0, limit=16):
    return pl.pallas_call(
        kernel,
        out_shape=outs,
        in_specs=[SM] * scalars + [VM] * (len(ins) - scalars),
        out_specs=out_specs or [VM] * len(outs),
        scratch_shapes=list(scratch),
        compiler_params=pltpu.CompilerParams(vmem_limit_bytes=limit * MIB),
    )(*ins)


def exchange(value, axes):
    return lax.all_to_all(value, axes, split_axis=0, concat_axis=0, tiled=True)


def shards(data, obs_points, src_points, obs_basis, src_basis, couplings, near_pairs, far_pairs):
    index = lax.axis_index(SRC).astype(jnp.int32)
    column = index.reshape(1)
    zone = (index % 4).reshape(1)
    near = near_pairs.reshape(-1)
    near_row = jnp.pad(near_pairs.reshape(1, -1), ((0, 0), (0, 56)), constant_values=-1)
    far_row = jnp.pad(far_pairs.reshape(1, -1), ((0, 0), (0, 64)), constant_values=-1)
    obs_message = shape(16, 8, 896)
    src_message = shape(8, 8, 384)
    row = shape(8, 128)

    (message,) = call(start_obs, [obs_message], [zone, data, obs_basis], scalars=1)
    received = exchange(message, SRC)

    def bf(*dims):
        return shape(*dims, dtype=BF16)

    kh, kl, pq, count, oo, oot, ost, os, fo, fot, fs, fst = call(
        setup_near,
        [
            bf(PAIRS, 256, 256), bf(PAIRS, 256, 256), shape(6, PAIRS, 256), shape(1, dtype=jnp.int32),
            bf(128, 16), bf(16, 128), bf(64, 128), bf(128, 64), bf(384, 128), bf(128, 384), bf(384, 64), bf(64, 384),
        ],
        [near, column, near_row, far_row, obs_points, src_points],
        scalars=2,
        out_specs=[VM] * 3 + [SM] + [VM] * 8,
        limit=28,
    )
    tile = pl.BlockSpec((1, 256, 256), lambda t: (t, 0, 0))
    wh, wl = pl.pallas_call(
        setup_far,
        grid=(20,),
        out_shape=[bf(20, 256, 256), bf(20, 256, 256)],
        in_specs=[pl.BlockSpec((16, 64, 64), lambda t: (t, 0, 0))],
        out_specs=[tile, tile],
        compiler_params=pltpu.CompilerParams(vmem_limit_bytes=16 * MIB),
    )(couplings.reshape(320, 64, 64))

    def adjoint(message):
        (out,) = call(
            adjoint_block,
            [shape(64, 384)],
            [count, column, message, kh, kl, pq, oo, ost, fo, fst, wh, wl],
            scalars=2,
            scratch=[
                pltpu.VMEM((16, 1536), F32), pltpu.VMEM((80, 1536), F32), pltpu.VMEM((2, 80 * ROWS, 128), F32),
                pltpu.VMEM((2, 80 * ROWS, 128), F32), pltpu.VMEM((128, 256), F32),
            ],
            limit=36,
        )
        return exchange(out.reshape(8, 8, 384), OBS)

    def forward(message):
        (out,) = call(
            forward_block,
            [obs_message],
            [count, column, exchange(message, OBS).reshape(64, 384), kh, kl, pq, os, oot, fs, fot, wh, wl],
            scalars=2,
            scratch=[
                pltpu.VMEM((80, 256), F32), pltpu.VMEM((2, 80 * ROWS, 128), F32), pltpu.VMEM((2, 80 * ROWS, 128), F32),
                pltpu.VMEM((128, 1536), F32), pltpu.VMEM((16, 1536), F32),
            ],
            limit=36,
        )
        return exchange(out, SRC)

    plane, line = shape(8, 1536), shape(8, 256)
    n0, sums0, message = call(first_src, [line, row, src_message], [adjoint(received), src_basis])
    p0, gamma0, message = call(
        first_obs, [plane, row, obs_message], [zone, forward(message), data, obs_basis], scalars=1
    )
    n1, sums1, message = call(
        second_src, [line, row, src_message], [adjoint(exchange(message, SRC)), src_basis, n0, gamma0]
    )
    p1, r1, gamma1, message = call(
        second_obs,
        [plane, plane, row, obs_message],
        [zone, forward(message), data, p0, gamma0, sums1, obs_basis],
        scalars=1,
    )
    found, residual, normal, misfit = call(
        last_src,
        [line, plane, line, row],
        [adjoint(exchange(message, SRC)), src_basis, n0, n1, gamma0, gamma1, sums0, sums1, r1, p1],
    )
    return found, residual, normal, misfit[0, 0:3]


def solution(mesh):
    finer = Mesh(mesh.devices.reshape(4, 2, 4, 4), ("obs_0", "obs_1", "src_0", "src_1"))
    return jax.shard_map(
        shards,
        mesh=finer,
        in_specs=(
            P(OBS_SRC, None),
            P(OBS, None, None),
            P(SRC, None, None),
            P(OBS_SRC, None, None),
            P(SRC_OBS, None, None),
            P(OBS, SRC, None, None, None),
            P(OBS, SRC, None),
            P(OBS, SRC, None),
        ),
        out_specs=(P(SRC_OBS, None), P(OBS_SRC, None), P(SRC_OBS, None), P()),
        check_vma=False,
    )
```

```python
import functools

import jax
import jax.numpy as jnp
from jax import lax
from jax.experimental import pallas as pl
from jax.experimental.pallas import tpu as pltpu
from jax.sharding import Mesh
from jax.sharding import PartitionSpec as P

OBS_SRC = ("obs_0", "obs_1", "src_0", "src_1")
SRC = ("src_0", "src_1")
OBS = ("obs_0", "obs_1")
SRC_OBS = ("src_0", "src_1", "obs_0", "obs_1")

F32 = jnp.float32
BF16 = jnp.bfloat16
PAIRS = 72
ROWS = 16
MIB = 1 << 20
LIMIT0 = 4
LIMIT = 10


def split(value):
    high = value.astype(BF16)
    return high, (value - high.astype(F32)).astype(BF16)


def mm(a, b):
    return lax.dot_general(a, b, (((1,), (0,)), ((), ())), preferred_element_type=F32)


def mm_nt(a, b):
    return lax.dot_general(a, b, (((1,), (1,)), ((), ())), preferred_element_type=F32)


def iota(shape, dim):
    return lax.broadcasted_iota(jnp.int32, shape, dim)


def lane_scalar(block, which):
    lanes = iota(block.shape, 1)
    return jnp.sum(jnp.where(lanes == 64 + which, block, 0.0), axis=1, keepdims=True)


def total(value):
    return jnp.sum(jnp.sum(value, axis=1, keepdims=True), axis=0, keepdims=True)


def with_scalars(block, scalars):
    lanes = iota(block.shape, 1)
    for which, value in enumerate(scalars):
        block = jnp.where(lanes == 64 + which, value, block)
    return block


def setup_near(slots, column, near, far, obs, src, kh, kl, pq, count, oo, oot, ost, os, fot, fst, near_row, far_row):
    j = column[0]
    near_row[...] = jnp.full_like(near_row, -1)
    near_row[:, 0:72] = near[...]
    far_row[...] = jnp.full_like(far_row, -1)
    far_row[:, 0:320] = far[...]
    f = near_row[...]
    live = f >= 0
    n = jnp.sum(jnp.where(live, 1.0, 0.0)).astype(jnp.int32)
    count[0] = n
    o = lax.shift_right_arithmetic(f, 6)
    s = jnp.where(live, f & 63, -1)
    oc = jnp.where(live, lax.shift_right_arithmetic(o, 5) * 4 + (o & 31) - (2 * j - 1), -1)
    a = (iota((16, 128), 0) == oc).astype(F32)
    oot[...] = a.astype(BF16)
    oo[...] = a.T.astype(BF16)
    a = (iota((64, 128), 0) == s).astype(F32)
    ost[...] = a.astype(BF16)
    os[...] = a.T.astype(BF16)
    f = far_row[...]
    live = f >= 0
    o = jnp.where(live, lax.shift_right_arithmetic(f, 6), -1)
    s = jnp.where(live, f & 63, -1)
    fot[...] = (iota((128, 384), 0) == o).astype(F32).astype(BF16)
    fst[...] = (iota((64, 384), 0) == s).astype(F32).astype(BF16)

    def eight(g, carry):
        for b in range(8):
            t = 8 * g + b
            name = jnp.maximum(slots[t], 0)
            for c in range(3):
                pq[c, pl.ds(t, 1), :] = obs[c, pl.ds(lax.shift_right_logical(name, 6), 1), :]
                pq[3 + c, pl.ds(t, 1), :] = src[c, pl.ds(name & 63, 1), :]
        at = pl.ds(pl.multiple_of(8 * g, 8), 8)
        p, q = [], []
        for c in range(3):
            pc, qc = pq[c, at, :], pq[3 + c, at, :]
            centre = 0.5 * (jnp.mean(pc, axis=1, keepdims=True) + jnp.mean(qc, axis=1, keepdims=True))
            pc, qc = pc - centre, qc - centre
            pq[c, at, :] = pc
            pq[3 + c, at, :] = qc
            p.append(pc.T)
            q.append(qc)

        def one(b):
            for r in range(0, 256, 32):
                dx, dy, dz = (p[c][r : r + 32, b : b + 1] - q[c][b : b + 1] for c in range(3))
                inverse = lax.rsqrt(dx * dx + dy * dy + dz * dz)
                square = inverse * inverse
                fifth = square * square * (inverse * (1.0 / 256.0))
                high, low = split(fifth)
                kh[8 * g + b, r : r + 32, :] = high
                kl[8 * g + b, r : r + 32, :] = low

        for b in range(4):
            one(b)

        @pl.when(n > 8 * g + 4)
        def _():
            for b in range(4, 8):
                one(b)

        return carry

    lax.fori_loop(0, lax.shift_right_logical(n + 7, 3), eight, 0)


def far_inputs(x, pick):
    high, low = split(x.T[0:64, :])
    return mm(high, pick) + mm(low, pick)


def far_outputs(terms, place):
    high, low = split(terms)
    return mm_nt(place, high) + mm_nt(place, low)


def far_forward(x, pick, place, c, terms):
    v = far_inputs(x, pick)[:, 0:320]
    terms[...] = jnp.zeros_like(terms)

    def eight(g, carry):
        rows = [jnp.sum(c[8 * g + b] * v, axis=0, keepdims=True) for b in range(8)]
        terms[pl.ds(pl.multiple_of(8 * g, 8), 8), 0:320] = jnp.concatenate(rows, axis=0)
        return carry

    lax.fori_loop(0, 8, eight, 0)
    return far_outputs(terms[...], place)


def far_adjoint(x, pick, place, c, terms, held):
    held[...] = far_inputs(x, pick)
    terms[...] = jnp.zeros_like(terms)

    def eight(g, carry):
        for b in range(8):
            carry = carry + c[8 * g + b] * held[pl.ds(8 * g + b, 1), 0:320]
        return carry

    terms[0:64, 0:320] = lax.fori_loop(0, 8, eight, jnp.zeros((64, 320), F32))
    return far_outputs(terms[...], place)


def near_products(n, moments, results, kh, kl, forward):
    def four(g, carry):
        for b in range(4):
            t = 4 * g + b
            at = pl.ds(pl.multiple_of(t * ROWS, ROWS), ROWS)
            high, low = split(jnp.concatenate([moments[0, at, :], moments[1, at, :]], axis=1))
            both = jnp.concatenate([high, low], axis=0)
            if forward:
                both = (mm_nt(kh[t], both) + mm_nt(kl[t], both)).T
            else:
                both = mm(both, kh[t]) + mm(both, kl[t])
            both = both[:ROWS] + both[ROWS:]
            results[0, at, :] = both[:, :128]
            results[1, at, :] = both[:, 128:]
        return carry

    lax.fori_loop(0, lax.shift_right_logical(n + 3, 2), four, 0)


def store_moment(moments, g, c, value):
    at = pl.ds(g * (8 * ROWS) + c, 8, ROWS)
    moments.at[0][at, :] = value[:, :128]
    moments.at[1][at, :] = value[:, 128:]


def load_result(results, g, c):
    at = pl.ds(g * (8 * ROWS) + c, 8, ROWS)
    return jnp.concatenate([results.at[0][at, :], results.at[1][at, :]], axis=1)


def adjoint_block(
    count, column, recv, kh, kl, pq, oo, ost, fot, fst, c, out, yb, yp, moments, results, values, terms, held
):
    n = count[0]
    j = column[0]
    for t in range(4):
        col = 2 * j - 1 + t
        inside = jnp.logical_and(col >= 0, col < 32)
        holder = lax.shift_right_logical(jnp.clip(col, 0, 31), 3)
        for row in range(4):
            for half in range(2):
                piece = recv[row * 4 + holder, 2 * t + half : 2 * t + half + 1, 0:768]
                if t in (0, 3):
                    piece = jnp.where(inside, piece, 0.0)
                yb[4 * row + t : 4 * row + t + 1, 768 * half : 768 * half + 768] = piece
    high, low = split(yb[...])
    yp[...] = mm(oo[0:80, :], high) + mm(oo[0:80, :], low)
    values[...] = jnp.zeros_like(values)
    groups = lax.shift_right_logical(n + 7, 3)

    def enter(g, carry):
        at = pl.ds(pl.multiple_of(g * 8, 8), 8)
        y = [yp[at, 256 * a : 256 * a + 256] for a in range(6)]
        px, py, pz = (pq[c, at, :] for c in range(3))
        trace = y[0] + y[3] + y[5]
        hxx, hyy, hzz = (3.0 * y[a] - trace for a in (0, 3, 5))
        hxy, hxz, hyz = (3.0 * y[a] for a in (1, 2, 4))
        ax, ay, az = hxx * px, hyy * py, hzz * pz
        bx, by, bz = hxy * py + hxz * pz, hxy * px + hyz * pz, hxz * px + hyz * py
        constant = px * (ax + hxy * py) + py * (ay + hyz * pz) + pz * (az + hxz * px)
        rows = (constant, 2.0 * ax + bx, 2.0 * ay + by, 2.0 * az + bz, hxx, hxy, hxz, hyy, hyz, hzz)
        for c, row in enumerate(rows):
            store_moment(moments, g, c, row)
        return carry

    lax.fori_loop(0, groups, enter, 0)
    near_products(n, moments, results, kh, kl, False)

    def leave(g, carry):
        at = pl.ds(pl.multiple_of(g * 8, 8), 8)
        w = [load_result(results, g, c) for c in range(10)]
        qx, qy, qz = (pq[3 + c, at, :] for c in range(3))
        z = w[0] + qx * (w[4] * qx + w[5] * qy - w[1]) + qy * (w[7] * qy + w[8] * qz - w[2])
        z = z + qz * (w[9] * qz + w[6] * qx - w[3])
        values[at, :] = jnp.where(iota((8, 256), 0) + g * 8 < n, z, 0.0)
        return carry

    lax.fori_loop(0, groups, leave, 0)
    high, low = split(values[...])
    out[:, 0:256] = mm(ost[...], high) + mm(ost[...], low)
    tails = [recv[k, :, 768:896] for k in range(16)]
    coeffs = far_adjoint(jnp.concatenate(tails, axis=0), fot[...], fst[...], c, terms, held)
    sums = functools.reduce(jnp.add, tails)
    for k in range(8):
        part = coeffs[8 * k : 8 * k + 8]
        out[8 * k : 8 * k + 8, 256:384] = jnp.where(iota((8, 128), 1) < 64, part, sums)


def forward_block(
    count, column, recv, kh, kl, pq, os, oot, fot, fst, c, out, xp, moments, results, values, yb, terms
):
    n = count[0]
    j = column[0]
    high, low = split(recv[:, 0:256])
    xp[...] = mm(os[0:80, :], high) + mm(os[0:80, :], low)
    values[...] = jnp.zeros_like(values)
    groups = lax.shift_right_logical(n + 7, 3)

    def enter(g, carry):
        at = pl.ds(pl.multiple_of(g * 8, 8), 8)
        x = xp[at, :]
        qx, qy, qz = (pq[3 + c, at, :] for c in range(3))
        x1, x2, x3 = x * qx, x * qy, x * qz
        rows = (x, x1, x2, x3, x1 * qx, x1 * qy, x1 * qz, x2 * qy, x2 * qz, x3 * qz)
        for c, row in enumerate(rows):
            store_moment(moments, g, c, row)
        return carry

    lax.fori_loop(0, groups, enter, 0)
    near_products(n, moments, results, kh, kl, True)

    def leave(g, carry):
        at = pl.ds(pl.multiple_of(g * 8, 8), 8)
        s = [load_result(results, g, c) for c in range(10)]
        px, py, pz = (pq[c, at, :] for c in range(3))
        ax, ay, az = px * s[0] - s[1], py * s[0] - s[2], pz * s[0] - s[3]
        xx = px * (ax - s[1]) + s[4]
        xy = py * ax - px * s[2] + s[5]
        xz = pz * ax - px * s[3] + s[6]
        yy = py * (ay - s[2]) + s[7]
        yz = pz * ay - py * s[3] + s[8]
        zz = pz * (az - s[3]) + s[9]
        trace = xx + yy + zz
        inside = iota((8, 256), 0) + g * 8 < n
        parts = (3.0 * xx - trace, 3.0 * xy, 3.0 * xz, 3.0 * yy - trace, 3.0 * yz, 3.0 * zz - trace)
        for a, part in enumerate(parts):
            values[at, 256 * a : 256 * a + 256] = jnp.where(inside, part, 0.0)
        return carry

    lax.fori_loop(0, groups, leave, 0)
    high, low = split(values[...])
    yb[...] = mm(oot[...], high) + mm(oot[...], low)
    for t in range(4):
        holder = lax.shift_right_logical(jnp.clip(2 * j - 1 + t, 0, 31), 3)
        for row in range(4):
            for half in range(2):
                piece = yb[4 * row + t : 4 * row + t + 1, 768 * half : 768 * half + 768]
                out[row * 4 + holder, 2 * t + half : 2 * t + half + 1, 0:768] = piece
    tails = [recv[8 * k : 8 * k + 8, 256:384] for k in range(8)]
    coeffs = far_forward(recv[:, 256:384], fst[...], fot[...], c, terms)
    sums = functools.reduce(jnp.add, tails)
    for k in range(16):
        out[k, :, 768:896] = jnp.where(iota((8, 128), 1) < 64, coeffs[8 * k : 8 * k + 8], sums)


def send_residual(zone, values, basis, out, scalars):
    lanes = iota((64, 128), 1)
    columns = jnp.zeros((64, 128), F32)
    for r in range(8):
        column = jnp.sum(basis[r] * values[r : r + 1, :], axis=1, keepdims=True)
        columns = jnp.where(lanes == r, column, columns)
    columns = jnp.concatenate([columns, jnp.zeros((64, 128), F32)], axis=0)
    tail = with_scalars(columns.T[0:8, :], scalars)
    for k in range(16):
        out[k, :, 768:896] = tail

    def rows(d):
        for t in range(4):
            r = 2 * d - 1 + t
            if 0 <= r < 8:
                for half in range(2):
                    piece = values[r : r + 1, 768 * half : 768 * half + 768]
                    out[4 * zone + d, 2 * t + half : 2 * t + half + 1, 0:768] = piece

    for d in range(4):
        rows(d)

    @pl.when(zone > 0)
    def _():
        rows(-1)

    @pl.when(zone < 3)
    def _():
        rows(4)


def start_obs(zone, count, data, basis, out):
    send_residual(zone[0], data, basis, out, (total(data[...] * data[...]),))


def gather_projected(zone, recv, basis, p):
    tail = functools.reduce(jnp.add, [recv[k, :, 768:896] for k in range(16)])
    columns = jnp.where(iota((8, 128), 1) < 64, tail, 0.0).T
    for r in range(8):
        far = jnp.sum(basis[r] * columns[0:64, r : r + 1], axis=0, keepdims=True)
        for half in range(2):
            value = far[:, 768 * half : 768 * half + 768]
            for t in range(4):
                if (r + 1 - t) % 2 == 0:
                    d = (r + 1 - t) // 2
                    piece = recv[jnp.clip(4 * zone + d, 0, 15), 2 * t + half : 2 * t + half + 1, 0:768]
                    if d == -1:
                        piece = jnp.where(zone > 0, piece, 0.0)
                    if d == 4:
                        piece = jnp.where(zone < 3, piece, 0.0)
                    value = value + piece
            p[r : r + 1, 768 * half : 768 * half + 768] = value
    return tail


def first_obs(zone, recv, data, basis, p, gammas, out):
    z = zone[0]
    gammas[...] = gather_projected(z, recv, basis, p)
    pv, dv = p[...], data[...]
    send_residual(z, p, basis, out, (total(pv * pv), total(dv * pv)))


def second_obs(zone, recv, data, p0, gamma0, sums1, basis, p, r, gammas, out):
    z = zone[0]
    tail = gather_projected(z, recv, basis, p)
    gammas[...] = tail
    g0 = lane_scalar(gamma0[...], 0)
    pv = p[...] + (lane_scalar(tail, 0) / g0) * p0[...]
    rv = data[...] - (g0 / lane_scalar(sums1[...], 0)) * p0[...]
    p[...] = pv
    r[...] = rv
    send_residual(z, p, basis, out, (total(pv * pv), total(rv * pv)))


def gather_normal(recv, basis, q):
    block = functools.reduce(jnp.add, [recv[k] for k in range(8)])
    tail = block[:, 256:384]
    columns = jnp.where(iota((8, 128), 1) < 64, tail, 0.0).T
    for r in range(8):
        far = jnp.sum(basis[r] * columns[0:64, r : r + 1], axis=0, keepdims=True)
        q[r : r + 1, :] = block[r : r + 1, 0:256] + far
    return tail


def send_direction(x, basis, out):
    lanes = iota((64, 128), 1)
    columns = jnp.zeros((64, 128), F32)
    for r in range(8):
        column = jnp.sum(basis[r] * x[r : r + 1], axis=1, keepdims=True)
        columns = jnp.where(lanes == r, column, columns)
    columns = jnp.concatenate([columns, jnp.zeros((64, 128), F32)], axis=0)
    tail = with_scalars(columns.T[0:8, :], (total(x * x),))
    for k in range(8):
        out[k, :, 0:256] = x
        out[k, :, 256:384] = tail


def first_src(recv, basis, n0, sums, out):
    sums[...] = gather_normal(recv, basis, n0)
    send_direction(n0[...], basis, out)


def second_src(recv, basis, n0, gamma0, n1, sums, out):
    tail = gather_normal(recv, basis, n1)
    sums[...] = tail
    x = n0[...] - (lane_scalar(gamma0[...], 0) / lane_scalar(tail, 0)) * n1[...]
    n1[...] = x
    send_direction(x, basis, out)


def last_src(recv, basis, n0, n1, gamma0, gamma1, sums0, sums1, r1, p1, found, residual, normal, misfit):
    tail = gather_normal(recv, basis, normal)
    g0, g1 = lane_scalar(gamma0[...], 0), lane_scalar(gamma1[...], 0)
    s1 = sums1[...]
    curve0, cross0 = lane_scalar(s1, 0), lane_scalar(s1, 1)
    curve1, cross1 = lane_scalar(tail, 0), lane_scalar(tail, 1)
    step0, step1 = g0 / curve0, g1 / curve1
    normal[...] = n1[...] - step1 * normal[...]
    found[...] = step0 * n0[...] + step1 * (n1[...] + (g1 / g0) * n0[...])
    residual[...] = r1[...] - step1 * p1[...]
    m0 = lane_scalar(sums0[...], 0)
    m1 = m0 - 2.0 * step0 * cross0 + step0 * step0 * curve0
    m2 = m1 - 2.0 * step1 * cross1 + step1 * step1 * curve1
    lanes = iota((8, 128), 1)
    misfit[...] = jnp.where(lanes == 0, m0, jnp.where(lanes == 1, m1, m2))


VM = pl.BlockSpec(memory_space=pltpu.VMEM)
SM = pl.BlockSpec(memory_space=pltpu.SMEM)


def shape(*dims, dtype=F32):
    return jax.ShapeDtypeStruct(dims, dtype)


def call(kernel, outs, ins, scratch=(), out_specs=None, scalars=0, limit=4):
    return pl.pallas_call(
        kernel,
        out_shape=outs,
        in_specs=[SM] * scalars + [VM] * (len(ins) - scalars),
        out_specs=out_specs or [VM] * len(outs),
        scratch_shapes=list(scratch),
        compiler_params=pltpu.CompilerParams(vmem_limit_bytes=limit * MIB),
    )(*ins)


def exchange(value, axes):
    return lax.all_to_all(value, axes, split_axis=0, concat_axis=0, tiled=True)


def shards(data, obs_points, src_points, obs_basis, src_basis, couplings, near_pairs, far_pairs):
    index = lax.axis_index(SRC).astype(jnp.int32)
    column = index.reshape(1)
    zone = (index % 4).reshape(1)
    near = near_pairs.reshape(-1)
    obs_message = shape(16, 8, 896)
    src_message = shape(8, 8, 384)
    row = shape(8, 128)

    def bf(*dims):
        return shape(*dims, dtype=BF16)

    kh, kl, pq, count, oo, oot, ost, os, fot, fst = call(
        setup_near,
        [
            bf(PAIRS, 256, 256), bf(PAIRS, 256, 256), shape(6, PAIRS, 256), shape(1, dtype=jnp.int32),
            bf(128, 16), bf(16, 128), bf(64, 128), bf(128, 64), bf(128, 384), bf(64, 384),
        ],
        [
            near, column, near_pairs.reshape(1, 72), far_pairs.reshape(1, 320),
            jnp.transpose(obs_points, (1, 0, 2)), jnp.transpose(src_points, (1, 0, 2)),
        ],
        scalars=2,
        out_specs=[VM] * 3 + [SM] + [VM] * 6,
        scratch=[pltpu.VMEM((1, 128), jnp.int32), pltpu.VMEM((1, 384), jnp.int32)],
        limit=LIMIT0,
    )
    matrices = jnp.transpose(couplings[0, 0], (1, 2, 0))
    (message,) = call(start_obs, [obs_message], [zone, count, data, obs_basis], scalars=2)
    received = exchange(message, SRC)

    def adjoint(message):
        (out,) = call(
            adjoint_block,
            [shape(64, 384)],
            [count, column, message, kh, kl, pq, oo, ost, fot, fst, matrices],
            scalars=2,
            scratch=[
                pltpu.VMEM((16, 1536), F32), pltpu.VMEM((80, 1536), F32), pltpu.VMEM((2, 80 * ROWS, 128), F32),
                pltpu.VMEM((2, 80 * ROWS, 128), F32), pltpu.VMEM((128, 256), F32), pltpu.VMEM((128, 384), F32),
                pltpu.VMEM((64, 384), F32),
            ],
            limit=LIMIT,
        )
        return exchange(out.reshape(8, 8, 384), OBS)

    def forward(message):
        (out,) = call(
            forward_block,
            [obs_message],
            [count, column, exchange(message, OBS).reshape(64, 384), kh, kl, pq, os, oot, fot, fst, matrices],
            scalars=2,
            scratch=[
                pltpu.VMEM((80, 256), F32), pltpu.VMEM((2, 80 * ROWS, 128), F32), pltpu.VMEM((2, 80 * ROWS, 128), F32),
                pltpu.VMEM((128, 1536), F32), pltpu.VMEM((16, 1536), F32), pltpu.VMEM((128, 384), F32),
            ],
            limit=LIMIT,
        )
        return exchange(out, SRC)

    plane, line = shape(8, 1536), shape(8, 256)
    n0, sums0, message = call(first_src, [line, row, src_message], [adjoint(received), src_basis])
    p0, gamma0, message = call(
        first_obs, [plane, row, obs_message], [zone, forward(message), data, obs_basis], scalars=1
    )
    n1, sums1, message = call(
        second_src, [line, row, src_message], [adjoint(exchange(message, SRC)), src_basis, n0, gamma0]
    )
    p1, r1, gamma1, message = call(
        second_obs,
        [plane, plane, row, obs_message],
        [zone, forward(message), data, p0, gamma0, sums1, obs_basis],
        scalars=1,
    )
    found, residual, normal, misfit = call(
        last_src,
        [line, plane, line, row],
        [adjoint(exchange(message, SRC)), src_basis, n0, n1, gamma0, gamma1, sums0, sums1, r1, p1],
    )
    return found, residual, normal, misfit[0, 0:3]


def solution(mesh):
    finer = Mesh(mesh.devices.reshape(4, 2, 4, 4), ("obs_0", "obs_1", "src_0", "src_1"))
    return jax.shard_map(
        shards,
        mesh=finer,
        in_specs=(
            P(OBS_SRC, None),
            P(OBS, None, None),
            P(SRC, None, None),
            P(OBS_SRC, None, None),
            P(SRC_OBS, None, None),
            P(OBS, SRC, None, None, None),
            P(OBS, SRC, None),
            P(OBS, SRC, None),
        ),
        out_specs=(P(SRC_OBS, None), P(OBS_SRC, None), P(SRC_OBS, None), P()),
        check_vma=False,
    )
```

```python
import functools

import jax
import jax.numpy as jnp
from jax import lax
from jax.experimental import pallas as pl
from jax.experimental.pallas import tpu as pltpu
from jax.sharding import Mesh
from jax.sharding import PartitionSpec as P

OBS_SRC = ("obs_0", "obs_1", "src_0", "src_1")
SRC = ("src_0", "src_1")
OBS = ("obs_0", "obs_1")
SRC_OBS = ("src_0", "src_1", "obs_0", "obs_1")

F32 = jnp.float32
BF16 = jnp.bfloat16
PAIRS = 72
ROWS = 16
MIB = 1 << 20
LIMIT0 = 8
LIMIT = 18


def split(value):
    high = value.astype(BF16)
    return high, (value - high.astype(F32)).astype(BF16)


def thirds(value):
    first = value.astype(BF16).astype(F32)
    rest = value - first
    second = rest.astype(BF16).astype(F32)
    return first, second, (rest - second).astype(BF16).astype(F32)


def mm(a, b):
    return lax.dot_general(a, b, (((1,), (0,)), ((), ())), preferred_element_type=F32)


def mm_nt(a, b):
    return lax.dot_general(a, b, (((1,), (1,)), ((), ())), preferred_element_type=F32)


def iota(shape, dim):
    return lax.broadcasted_iota(jnp.int32, shape, dim)


def lane_scalar(block, which):
    lanes = iota(block.shape, 1)
    return jnp.sum(jnp.where(lanes == 64 + which, block, 0.0), axis=1, keepdims=True)


def total(value):
    return jnp.sum(jnp.sum(value, axis=1, keepdims=True), axis=0, keepdims=True)


def with_scalars(block, scalars):
    lanes = iota(block.shape, 1)
    for which, value in enumerate(scalars):
        block = jnp.where(lanes == 64 + which, value, block)
    return block


def setup_near(
    column, near, far, obs, src, kh, kl, pq, count, oo, oot, ost, os, fot, fst,
    slots, near_part, far_part, near_row, far_row, points, sources, left, right, built, sems, out_sems
):
    copies = [
        pltpu.make_async_copy(a, b, sems.at[k])
        for k, (a, b) in enumerate(
            ((near, slots), (near, near_part), (far, far_part), (obs, points), (src, sources))
        )
    ]
    for copy in copies:
        copy.start()
    j = column[0]
    near_row[...] = jnp.full_like(near_row, -1)
    far_row[...] = jnp.full_like(far_row, -1)
    left[...] = jnp.zeros_like(left)
    right[...] = jnp.zeros_like(right)
    for copy in copies:
        copy.wait()
    near_row[:, 0:72] = near_part[...]
    far_row[:, 0:320] = far_part[...]
    f = near_row[...]
    live = f >= 0
    n = jnp.sum(jnp.where(live, 1.0, 0.0)).astype(jnp.int32)
    count[0] = n
    count[1] = jnp.sum(jnp.where(far_row[...] >= 0, 1.0, 0.0)).astype(jnp.int32)
    o = lax.shift_right_arithmetic(f, 6)
    s = jnp.where(live, f & 63, -1)
    oc = jnp.where(live, lax.shift_right_arithmetic(o, 5) * 4 + (o & 31) - (2 * j - 1), -1)
    a = (iota((16, 128), 0) == oc).astype(F32)
    oot[...] = a.astype(BF16)
    oo[...] = a.T.astype(BF16)
    a = (iota((64, 128), 0) == s).astype(F32)
    ost[...] = a.astype(BF16)
    os[...] = a.T.astype(BF16)
    f = far_row[...]
    live = f >= 0
    o = jnp.where(live, lax.shift_right_arithmetic(f, 6), -1)
    s = jnp.where(live, f & 63, -1)
    fot[...] = (iota((128, 384), 0) == o).astype(F32).astype(BF16)
    fst[...] = (iota((64, 384), 0) == s).astype(F32).astype(BF16)
    groups = lax.shift_right_logical(n + 7, 3)

    def leaving(g):
        at = pl.ds(8 * g, 8)
        return [
            pltpu.make_async_copy(built.at[g & 1, k], out.at[at], out_sems.at[g & 1, k])
            for k, out in enumerate((kh, kl))
        ]

    def eight(g, carry):
        @pl.when(g >= 2)
        def _():
            for copy in leaving(g - 2):
                copy.wait()

        def one(b):
            t = 8 * g + b
            name = jnp.maximum(slots[0, t], 0)
            own = slice(8 * b, 8 * b + 8)
            for c in range(3):
                left[8 * b + c : 8 * b + c + 1, :] = points[c, pl.ds(lax.shift_right_logical(name, 6), 1), :]
                right[8 * b + c : 8 * b + c + 1, :] = sources[c, pl.ds(name & 63, 1), :]
            p, q = left[own, :], right[own, :]
            centre = 0.5 * (jnp.mean(p, axis=1, keepdims=True) + jnp.mean(q, axis=1, keepdims=True))
            p, q = p - centre, q - centre
            for c in range(3):
                pq[c, pl.ds(t, 1), :] = p[c : c + 1]
                pq[3 + c, pl.ds(t, 1), :] = q[c : c + 1]
            p1, p2, p3 = thirds(p)
            q1, q2, q3 = thirds(-2.0 * q)
            at = iota((8, 256), 0)
            end_p = jnp.where(at < 6, 1.0, 0.0)
            end_q = end_p
            for k, (x, y) in enumerate(
                zip(
                    thirds(jnp.sum(p * p, axis=0, keepdims=True)),
                    thirds(jnp.sum(q * q, axis=0, keepdims=True)),
                )
            ):
                end_p = jnp.where(at == k, x, end_p)
                end_q = jnp.where(at == k + 3, y, end_q)
            factor_p = jnp.concatenate([p1, p1, p2, p2, p1, p3, end_p, jnp.zeros((8, 256), F32)], axis=0)
            factor_q = jnp.concatenate([q1, q2, q1, q2, q3, q1, end_q, jnp.zeros((8, 256), F32)], axis=0)
            factor_q = factor_q.astype(BF16)
            factor_p = factor_p.T.astype(BF16)
            for r in range(0, 256, 64):
                inverse = lax.rsqrt(mm(factor_p[r : r + 64], factor_q))
                square = inverse * inverse
                high, low = split(square * square * inverse)
                built[g & 1, 0, b, r : r + 64, :] = high
                built[g & 1, 1, b, r : r + 64, :] = low

        for b in range(4):
            one(b)

        @pl.when(n > 8 * g + 4)
        def _():
            for b in range(4, 8):
                one(b)

        for copy in leaving(g):
            copy.start()
        return carry

    lax.fori_loop(0, groups, eight, 0)
    for back in (2, 1):

        @pl.when(groups >= back)
        def _():
            for copy in leaving(groups - back):
                copy.wait()


def far_inputs(x, pick):
    high, low = split(x.T[0:64, :])
    return mm(high, pick) + mm(low, pick)


def far_outputs(terms, place):
    high, low = split(terms)
    return mm_nt(place, high) + mm_nt(place, low)


WIDE = 256


def far_copies(n, c, matrices, sem, act):
    @pl.when(n <= WIDE)
    def _():
        act(pltpu.make_async_copy(c.at[:, :, pl.ds(0, WIDE)], matrices.at[:, :, pl.ds(0, WIDE)], sem))

    @pl.when(n > WIDE)
    def _():
        act(pltpu.make_async_copy(c, matrices, sem))


def far_forward(n, x, pick, place, c, terms):
    v = far_inputs(x, pick)
    terms[...] = jnp.zeros_like(terms)

    def part(lanes):
        def eight(g, carry):
            rows = [jnp.sum(c[8 * g + b, :, lanes] * v[:, lanes], axis=0, keepdims=True) for b in range(8)]
            terms[pl.ds(pl.multiple_of(8 * g, 8), 8), lanes] = jnp.concatenate(rows, axis=0)
            return carry

        lax.fori_loop(0, 8, eight, 0)

    part(slice(0, WIDE))

    @pl.when(n > WIDE)
    def _():
        part(slice(WIDE, 320))

    return far_outputs(terms[...], place)


def far_adjoint(n, x, pick, place, c, terms, held):
    held[...] = far_inputs(x, pick)
    terms[...] = jnp.zeros_like(terms)

    def part(lanes):
        def eight(g, carry):
            rows = held[pl.ds(pl.multiple_of(8 * g, 8), 8), lanes.start : (lanes.stop + 127) // 128 * 128]
            for b in range(8):
                carry = carry + c[8 * g + b, :, lanes] * rows[b : b + 1, 0 : lanes.stop - lanes.start]
            return carry

        zeros = jnp.zeros((64, lanes.stop - lanes.start), F32)
        terms[0:64, lanes] = lax.fori_loop(0, 8, eight, zeros)

    part(slice(0, WIDE))

    @pl.when(n > WIDE)
    def _():
        part(slice(WIDE, 320))

    return far_outputs(terms[...], place)


def near_products(n, moments, results, kh, kl, forward, arrive=None):
    def four(first):
        for b in range(4):
            t = first + b
            at = pl.ds(pl.multiple_of(t * ROWS, ROWS), ROWS)
            high, low = split(jnp.concatenate([moments[0, at, :], moments[1, at, :]], axis=1))
            both = jnp.concatenate([high, low], axis=0)
            if forward:
                both = (mm_nt(kh[t], both) + mm_nt(kl[t], both)).T
            else:
                both = mm(both, kh[t]) + mm(both, kl[t])
            both = both[:ROWS] + both[ROWS:]
            results[0, at, :] = both[:, :128]
            results[1, at, :] = both[:, 128:]

    def eight(g, carry):
        if arrive is not None:
            arrive(g)
        four(8 * g)
        four(8 * g + 4)
        return carry

    whole = lax.shift_right_logical(n, 3)
    lax.fori_loop(0, whole, eight, 0)

    @pl.when((n & 7) > 0)
    def _():
        if arrive is not None:
            arrive(whole)
        four(8 * whole)

        @pl.when((n & 7) > 4)
        def _():
            four(8 * whole + 4)


def store_moment(moments, g, c, value):
    at = pl.ds(g * (8 * ROWS) + c, 8, ROWS)
    moments.at[0][at, :] = value[:, :128]
    moments.at[1][at, :] = value[:, 128:]


def load_result(results, g, c):
    at = pl.ds(g * (8 * ROWS) + c, 8, ROWS)
    return jnp.concatenate([results.at[0][at, :], results.at[1][at, :]], axis=1)


def first_adjoint_block(
    count, column, recv, kh_far, kl_far, pq, oo, ost, fot, fst, c, out, kh, kl,
    yb, yp, moments, results, values, terms, held, matrices, sem, sems
):
    n = count[0]

    def arriving(g):
        at = pl.ds(8 * g, 8)
        return [
            pltpu.make_async_copy(a.at[at], b.at[at], sems.at[k, g])
            for k, (a, b) in enumerate(((kh_far, kh), (kl_far, kl)))
        ]

    def start(g, carry):
        for copy in arriving(g):
            copy.start()
        return carry

    def arrive(g):
        for copy in arriving(g):
            copy.wait()

    lax.fori_loop(0, lax.shift_right_logical(n + 7, 3), start, 0)
    adjoint_block(
        count, column, recv, kh, kl, pq, oo, ost, fot, fst, c, out,
        yb, yp, moments, results, values, terms, held, matrices, sem, arrive=arrive
    )


def adjoint_block(
    count, column, recv, kh, kl, pq, oo, ost, fot, fst, c, out,
    yb, yp, moments, results, values, terms, held, matrices, sem, arrive=None
):
    far_copies(count[1], c, matrices, sem, lambda copy: copy.start())
    n = count[0]
    j = column[0]
    for t in range(4):
        col = 2 * j - 1 + t
        inside = jnp.logical_and(col >= 0, col < 32)
        holder = lax.shift_right_logical(jnp.clip(col, 0, 31), 3)
        for row in range(4):
            for half in range(2):
                piece = recv[row * 4 + holder, 2 * t + half : 2 * t + half + 1, 0:768]
                if t in (0, 3):
                    piece = jnp.where(inside, piece, 0.0)
                yb[4 * row + t : 4 * row + t + 1, 768 * half : 768 * half + 768] = piece
    high, low = split(yb[...])
    yp[...] = mm(oo[0:80, :], high) + mm(oo[0:80, :], low)
    values[...] = jnp.zeros_like(values)
    groups = lax.shift_right_logical(n + 7, 3)

    def enter(g, carry):
        at = pl.ds(pl.multiple_of(g * 8, 8), 8)
        y = [yp[at, 256 * a : 256 * a + 256] for a in range(6)]
        px, py, pz = (pq[c, at, :] for c in range(3))
        trace = y[0] + y[3] + y[5]
        hxx, hyy, hzz = (3.0 * y[a] - trace for a in (0, 3, 5))
        hxy, hxz, hyz = (3.0 * y[a] for a in (1, 2, 4))
        ax, ay, az = hxx * px, hyy * py, hzz * pz
        bx, by, bz = hxy * py + hxz * pz, hxy * px + hyz * pz, hxz * px + hyz * py
        constant = px * (ax + hxy * py) + py * (ay + hyz * pz) + pz * (az + hxz * px)
        rows = (constant, 2.0 * ax + bx, 2.0 * ay + by, 2.0 * az + bz, hxx, hxy, hxz, hyy, hyz, hzz)
        for c, row in enumerate(rows):
            store_moment(moments, g, c, row)
        return carry

    lax.fori_loop(0, groups, enter, 0)
    near_products(n, moments, results, kh, kl, False, arrive)

    def leave(g, carry):
        at = pl.ds(pl.multiple_of(g * 8, 8), 8)
        w = [load_result(results, g, c) for c in range(10)]
        qx, qy, qz = (pq[3 + c, at, :] for c in range(3))
        z = w[0] + qx * (w[4] * qx + w[5] * qy - w[1]) + qy * (w[7] * qy + w[8] * qz - w[2])
        z = z + qz * (w[9] * qz + w[6] * qx - w[3])
        values[at, :] = jnp.where(iota((8, 256), 0) + g * 8 < n, z * (1.0 / 256.0), 0.0)
        return carry

    lax.fori_loop(0, groups, leave, 0)
    high, low = split(values[...])
    out[:, 0:256] = mm(ost[...], high) + mm(ost[...], low)
    tails = [recv[k, :, 768:896] for k in range(16)]
    far_copies(count[1], c, matrices, sem, lambda copy: copy.wait())
    coeffs = far_adjoint(count[1], jnp.concatenate(tails, axis=0), fot[...], fst[...], matrices, terms, held)
    sums = functools.reduce(jnp.add, tails)
    for k in range(8):
        part = coeffs[8 * k : 8 * k + 8]
        out[8 * k : 8 * k + 8, 256:384] = jnp.where(iota((8, 128), 1) < 64, part, sums)


def forward_block(
    count, column, recv, kh, kl, pq, os, oot, fot, fst, c, out,
    xp, moments, results, values, yb, terms, matrices, sem
):
    far_copies(count[1], c, matrices, sem, lambda copy: copy.start())
    n = count[0]
    j = column[0]
    high, low = split(recv[:, 0:256])
    xp[...] = mm(os[0:80, :], high) + mm(os[0:80, :], low)
    values[...] = jnp.zeros_like(values)
    groups = lax.shift_right_logical(n + 7, 3)

    def enter(g, carry):
        at = pl.ds(pl.multiple_of(g * 8, 8), 8)
        x = xp[at, :]
        qx, qy, qz = (pq[3 + c, at, :] for c in range(3))
        x1, x2, x3 = x * qx, x * qy, x * qz
        rows = (x, x1, x2, x3, x1 * qx, x1 * qy, x1 * qz, x2 * qy, x2 * qz, x3 * qz)
        for c, row in enumerate(rows):
            store_moment(moments, g, c, row)
        return carry

    lax.fori_loop(0, groups, enter, 0)
    near_products(n, moments, results, kh, kl, True)

    def leave(g, carry):
        at = pl.ds(pl.multiple_of(g * 8, 8), 8)
        s = [load_result(results, g, c) for c in range(10)]
        px, py, pz = (pq[c, at, :] for c in range(3))
        ax, ay, az = px * s[0] - s[1], py * s[0] - s[2], pz * s[0] - s[3]
        xx = px * (ax - s[1]) + s[4]
        xy = py * ax - px * s[2] + s[5]
        xz = pz * ax - px * s[3] + s[6]
        yy = py * (ay - s[2]) + s[7]
        yz = pz * ay - py * s[3] + s[8]
        zz = pz * (az - s[3]) + s[9]
        trace = xx + yy + zz
        inside = iota((8, 256), 0) + g * 8 < n
        parts = (3.0 * xx - trace, 3.0 * xy, 3.0 * xz, 3.0 * yy - trace, 3.0 * yz, 3.0 * zz - trace)
        for a, part in enumerate(parts):
            values[at, 256 * a : 256 * a + 256] = jnp.where(inside, part * (1.0 / 256.0), 0.0)
        return carry

    lax.fori_loop(0, groups, leave, 0)
    high, low = split(values[...])
    yb[...] = mm(oot[...], high) + mm(oot[...], low)
    for t in range(4):
        holder = lax.shift_right_logical(jnp.clip(2 * j - 1 + t, 0, 31), 3)
        for row in range(4):
            for half in range(2):
                piece = yb[4 * row + t : 4 * row + t + 1, 768 * half : 768 * half + 768]
                out[row * 4 + holder, 2 * t + half : 2 * t + half + 1, 0:768] = piece
    tails = [recv[8 * k : 8 * k + 8, 256:384] for k in range(8)]
    far_copies(count[1], c, matrices, sem, lambda copy: copy.wait())
    coeffs = far_forward(count[1], recv[:, 256:384], fst[...], fot[...], matrices, terms)
    sums = functools.reduce(jnp.add, tails)
    for k in range(16):
        out[k, :, 768:896] = jnp.where(iota((8, 128), 1) < 64, coeffs[8 * k : 8 * k + 8], sums)


def send_residual(zone, values, basis, out, scalars, copies=()):
    lanes = iota((64, 128), 1)
    columns = jnp.zeros((64, 128), F32)
    for r in range(8):
        if copies:
            copies[r].wait()
        column = jnp.sum(basis[r] * values[r : r + 1, :], axis=1, keepdims=True)
        columns = jnp.where(lanes == r, column, columns)
    columns = jnp.concatenate([columns, jnp.zeros((64, 128), F32)], axis=0)
    tail = with_scalars(columns.T[0:8, :], scalars)
    for k in range(16):
        out[k, :, 768:896] = tail

    def rows(d):
        for t in range(4):
            r = 2 * d - 1 + t
            if 0 <= r < 8:
                for half in range(2):
                    piece = values[r : r + 1, 768 * half : 768 * half + 768]
                    out[4 * zone + d, 2 * t + half : 2 * t + half + 1, 0:768] = piece

    for d in range(4):
        rows(d)

    @pl.when(zone > 0)
    def _():
        rows(-1)

    @pl.when(zone < 3)
    def _():
        rows(4)


def start_obs(zone, data_far, basis_far, out, data, basis, sem, sems):
    first = pltpu.make_async_copy(data_far, data, sem)
    first.start()
    copies = [pltpu.make_async_copy(basis_far.at[r], basis.at[r], sems.at[r]) for r in range(8)]
    for copy in copies:
        copy.start()
    first.wait()
    send_residual(zone[0], data, basis, out, (total(data[...] * data[...]),), copies)


def gather_projected(zone, recv, basis, p):
    tail = functools.reduce(jnp.add, [recv[k, :, 768:896] for k in range(16)])
    columns = jnp.where(iota((8, 128), 1) < 64, tail, 0.0).T
    for r in range(8):
        far = jnp.sum(basis[r] * columns[0:64, r : r + 1], axis=0, keepdims=True)
        for half in range(2):
            value = far[:, 768 * half : 768 * half + 768]
            for t in range(4):
                if (r + 1 - t) % 2 == 0:
                    d = (r + 1 - t) // 2
                    piece = recv[jnp.clip(4 * zone + d, 0, 15), 2 * t + half : 2 * t + half + 1, 0:768]
                    if d == -1:
                        piece = jnp.where(zone > 0, piece, 0.0)
                    if d == 4:
                        piece = jnp.where(zone < 3, piece, 0.0)
                    value = value + piece
            p[r : r + 1, 768 * half : 768 * half + 768] = value
    return tail


def first_obs(zone, recv, data, basis, p, gammas, out):
    z = zone[0]
    gammas[...] = gather_projected(z, recv, basis, p)
    pv, dv = p[...], data[...]
    send_residual(z, p, basis, out, (total(pv * pv), total(dv * pv)))


def second_obs(zone, recv, data, p0, gamma0, sums1, basis, p, r, gammas, out):
    z = zone[0]
    tail = gather_projected(z, recv, basis, p)
    gammas[...] = tail
    g0 = lane_scalar(gamma0[...], 0)
    pv = p[...] + (lane_scalar(tail, 0) / g0) * p0[...]
    rv = data[...] - (g0 / lane_scalar(sums1[...], 0)) * p0[...]
    p[...] = pv
    r[...] = rv
    send_residual(z, p, basis, out, (total(pv * pv), total(rv * pv)))


def gather_normal(recv, basis, q):
    block = functools.reduce(jnp.add, [recv[k] for k in range(8)])
    tail = block[:, 256:384]
    columns = jnp.where(iota((8, 128), 1) < 64, tail, 0.0).T
    for r in range(8):
        far = jnp.sum(basis[r] * columns[0:64, r : r + 1], axis=0, keepdims=True)
        q[r : r + 1, :] = block[r : r + 1, 0:256] + far
    return tail


def send_direction(x, basis, out):
    lanes = iota((64, 128), 1)
    columns = jnp.zeros((64, 128), F32)
    for r in range(8):
        column = jnp.sum(basis[r] * x[r : r + 1], axis=1, keepdims=True)
        columns = jnp.where(lanes == r, column, columns)
    columns = jnp.concatenate([columns, jnp.zeros((64, 128), F32)], axis=0)
    tail = with_scalars(columns.T[0:8, :], (total(x * x),))
    for k in range(8):
        out[k, :, 0:256] = x
        out[k, :, 256:384] = tail


def first_src(recv, basis, n0, sums, out):
    sums[...] = gather_normal(recv, basis, n0)
    send_direction(n0[...], basis, out)


def second_src(recv, basis, n0, gamma0, n1, sums, out):
    tail = gather_normal(recv, basis, n1)
    sums[...] = tail
    x = n0[...] - (lane_scalar(gamma0[...], 0) / lane_scalar(tail, 0)) * n1[...]
    n1[...] = x
    send_direction(x, basis, out)


def last_src(recv, basis, n0, n1, gamma0, gamma1, sums0, sums1, r1, p1, found, residual, normal, misfit):
    tail = gather_normal(recv, basis, normal)
    g0, g1 = lane_scalar(gamma0[...], 0), lane_scalar(gamma1[...], 0)
    s1 = sums1[...]
    curve0, cross0 = lane_scalar(s1, 0), lane_scalar(s1, 1)
    curve1, cross1 = lane_scalar(tail, 0), lane_scalar(tail, 1)
    step0, step1 = g0 / curve0, g1 / curve1
    normal[...] = n1[...] - step1 * normal[...]
    found[...] = step0 * n0[...] + step1 * (n1[...] + (g1 / g0) * n0[...])
    residual[...] = r1[...] - step1 * p1[...]
    m0 = lane_scalar(sums0[...], 0)
    m1 = m0 - 2.0 * step0 * cross0 + step0 * step0 * curve0
    m2 = m1 - 2.0 * step1 * cross1 + step1 * step1 * curve1
    lanes = iota((8, 128), 1)
    misfit[...] = jnp.where(lanes == 0, m0, jnp.where(lanes == 1, m1, m2))


VM = pl.BlockSpec(memory_space=pltpu.VMEM)
SM = pl.BlockSpec(memory_space=pltpu.SMEM)
FAR = pl.BlockSpec(memory_space=pltpu.HBM)


def shape(*dims, dtype=F32):
    return jax.ShapeDtypeStruct(dims, dtype)


def call(kernel, outs, ins, scratch=(), out_specs=None, scalars=0, far=(), limit=4):
    specs = [SM] * scalars + [VM] * (len(ins) - scalars)
    for at in far:
        specs[at] = FAR
    ins = [pltpu.with_memory_space_constraint(a, pltpu.HBM) if k in far else a for k, a in enumerate(ins)]
    return pl.pallas_call(
        kernel,
        out_shape=outs,
        in_specs=specs,
        out_specs=out_specs or [VM] * len(outs),
        scratch_shapes=list(scratch),
        compiler_params=pltpu.CompilerParams(vmem_limit_bytes=limit * MIB),
    )(*ins)


def exchange(value, axes):
    return lax.all_to_all(value, axes, split_axis=0, concat_axis=0, tiled=True)


def shards(data, obs_points, src_points, obs_basis, src_basis, couplings, near_pairs, far_pairs):
    index = lax.axis_index(SRC).astype(jnp.int32)
    column = index.reshape(1)
    zone = (index % 4).reshape(1)
    obs_message = shape(16, 8, 896)
    src_message = shape(8, 8, 384)
    row = shape(8, 128)
    dma = pltpu.SemaphoreType.DMA

    def bf(*dims):
        return shape(*dims, dtype=BF16)

    (message,) = call(
        start_obs,
        [obs_message],
        [zone, data, obs_basis],
        scalars=1,
        far=(1, 2),
        scratch=[pltpu.VMEM((8, 1536), F32), pltpu.VMEM((8, 64, 1536), F32), dma, dma((8,))],
        limit=LIMIT0,
    )
    received = exchange(message, SRC)
    kh_far, kl_far, pq, count, oo, oot, ost, os, fot, fst = call(
        setup_near,
        [
            *[pltpu.HBM((PAIRS, 256, 256), BF16)] * 2, shape(6, PAIRS, 256), shape(2, dtype=jnp.int32),
            bf(128, 16), bf(16, 128), bf(64, 128), bf(128, 64), bf(128, 384), bf(64, 384),
        ],
        [
            column, near_pairs.reshape(1, 72), far_pairs.reshape(1, 320),
            jnp.transpose(obs_points, (1, 0, 2)), jnp.transpose(src_points, (1, 0, 2)),
        ],
        scalars=1,
        far=(1, 2, 3, 4),
        out_specs=[FAR] * 2 + [VM] + [SM] + [VM] * 6,
        scratch=[
            pltpu.SMEM((1, 72), jnp.int32), pltpu.VMEM((1, 72), jnp.int32), pltpu.VMEM((1, 320), jnp.int32),
            pltpu.VMEM((1, 128), jnp.int32), pltpu.VMEM((1, 384), jnp.int32), pltpu.VMEM((3, 128, 256), F32),
            pltpu.VMEM((3, 64, 256), F32), pltpu.VMEM((64, 256), F32), pltpu.VMEM((64, 256), F32),
            pltpu.VMEM((2, 2, 8, 256, 256), BF16), dma((5,)), dma((2, 2)),
        ],
        limit=LIMIT0,
    )
    matrices = jnp.transpose(couplings[0, 0], (1, 2, 0))
    matrix_scratch = [pltpu.VMEM((64, 64, 320), F32), dma]
    adjoint_scratch = [
        pltpu.VMEM((16, 1536), F32), pltpu.VMEM((80, 1536), F32), pltpu.VMEM((2, 80 * ROWS, 128), F32),
        pltpu.VMEM((2, 80 * ROWS, 128), F32), pltpu.VMEM((128, 256), F32), pltpu.VMEM((128, 384), F32),
        pltpu.VMEM((64, 384), F32), *matrix_scratch,
    ]
    out, kh, kl = call(
        first_adjoint_block,
        [shape(64, 384), bf(PAIRS, 256, 256), bf(PAIRS, 256, 256)],
        [count, column, received, kh_far, kl_far, pq, oo, ost, fot, fst, matrices],
        scalars=2,
        far=(3, 4, 10),
        scratch=[*adjoint_scratch, dma((2, 9))],
        limit=LIMIT,
    )
    received = exchange(out.reshape(8, 8, 384), OBS)

    def adjoint(message):
        (out,) = call(
            adjoint_block,
            [shape(64, 384)],
            [count, column, message, kh, kl, pq, oo, ost, fot, fst, matrices],
            scalars=2,
            far=(10,),
            scratch=adjoint_scratch,
            limit=LIMIT,
        )
        return exchange(out.reshape(8, 8, 384), OBS)

    def forward(message):
        (out,) = call(
            forward_block,
            [obs_message],
            [count, column, exchange(message, OBS).reshape(64, 384), kh, kl, pq, os, oot, fot, fst, matrices],
            scalars=2,
            far=(10,),
            scratch=[
                pltpu.VMEM((80, 256), F32), pltpu.VMEM((2, 80 * ROWS, 128), F32), pltpu.VMEM((2, 80 * ROWS, 128), F32),
                pltpu.VMEM((128, 1536), F32), pltpu.VMEM((16, 1536), F32), pltpu.VMEM((128, 384), F32),
                *matrix_scratch,
            ],
            limit=LIMIT,
        )
        return exchange(out, SRC)

    plane, line = shape(8, 1536), shape(8, 256)
    n0, sums0, message = call(first_src, [line, row, src_message], [received, src_basis])
    p0, gamma0, message = call(
        first_obs, [plane, row, obs_message], [zone, forward(message), data, obs_basis], scalars=1
    )
    n1, sums1, message = call(
        second_src, [line, row, src_message], [adjoint(exchange(message, SRC)), src_basis, n0, gamma0]
    )
    p1, r1, gamma1, message = call(
        second_obs,
        [plane, plane, row, obs_message],
        [zone, forward(message), data, p0, gamma0, sums1, obs_basis],
        scalars=1,
    )
    found, residual, normal, misfit = call(
        last_src,
        [line, plane, line, row],
        [adjoint(exchange(message, SRC)), src_basis, n0, n1, gamma0, gamma1, sums0, sums1, r1, p1],
    )
    return found, residual, normal, misfit[0, 0:3]


def solution(mesh):
    finer = Mesh(mesh.devices.reshape(4, 2, 4, 4), ("obs_0", "obs_1", "src_0", "src_1"))
    return jax.shard_map(
        shards,
        mesh=finer,
        in_specs=(
            P(OBS_SRC, None),
            P(OBS, None, None),
            P(SRC, None, None),
            P(OBS_SRC, None, None),
            P(SRC_OBS, None, None),
            P(OBS, SRC, None, None, None),
            P(OBS, SRC, None),
            P(OBS, SRC, None),
        ),
        out_specs=(P(SRC_OBS, None), P(OBS_SRC, None), P(SRC_OBS, None), P()),
        check_vma=False,
    )
```

```python
import functools

import jax
import jax.numpy as jnp
from jax import lax
from jax.experimental import pallas as pl
from jax.experimental.pallas import tpu as pltpu
from jax.sharding import Mesh
from jax.sharding import PartitionSpec as P

OBS_SRC = ("obs_0", "obs_1", "src_0", "src_1")
SRC = ("src_0", "src_1")
OBS = ("obs_0", "obs_1")
SRC_OBS = ("src_0", "src_1", "obs_0", "obs_1")

F32 = jnp.float32
BF16 = jnp.bfloat16
PAIRS = 72
ROWS = 16
MIB = 1 << 20
LIMIT0 = 8
LIMIT = 18


def split(value):
    high = value.astype(BF16)
    return high, (value - high.astype(F32)).astype(BF16)


def thirds(value):
    first = value.astype(BF16).astype(F32)
    rest = value - first
    second = rest.astype(BF16).astype(F32)
    return first, second, (rest - second).astype(BF16).astype(F32)


def mm(a, b):
    return lax.dot_general(a, b, (((1,), (0,)), ((), ())), preferred_element_type=F32)


def mm_nt(a, b):
    return lax.dot_general(a, b, (((1,), (1,)), ((), ())), preferred_element_type=F32)


def iota(shape, dim):
    return lax.broadcasted_iota(jnp.int32, shape, dim)


def lane_scalar(block, which):
    lanes = iota(block.shape, 1)
    return jnp.sum(jnp.where(lanes == 64 + which, block, 0.0), axis=1, keepdims=True)


def total(value):
    return jnp.sum(jnp.sum(value, axis=1, keepdims=True), axis=0, keepdims=True)


def with_scalars(block, scalars):
    lanes = iota(block.shape, 1)
    for which, value in enumerate(scalars):
        block = jnp.where(lanes == 64 + which, value, block)
    return block


def setup_near(
    column, near, far, points, sources, kh, kl, pq, count, oo, oot, ost, os, fot, fst,
    slots, near_part, far_part, near_row, far_row, left, right, built, sems, out_sems
):
    copies = [
        pltpu.make_async_copy(a, b, sems.at[k])
        for k, (a, b) in enumerate(
            ((near, slots), (near, near_part), (far, far_part))
        )
    ]
    for copy in copies:
        copy.start()
    j = column[0]
    near_row[...] = jnp.full_like(near_row, -1)
    far_row[...] = jnp.full_like(far_row, -1)
    left[...] = jnp.zeros_like(left)
    right[...] = jnp.zeros_like(right)
    for copy in copies:
        copy.wait()
    near_row[:, 0:72] = near_part[...]
    far_row[:, 0:320] = far_part[...]
    f = near_row[...]
    live = f >= 0
    n = jnp.sum(jnp.where(live, 1.0, 0.0)).astype(jnp.int32)
    count[0] = n
    count[1] = jnp.sum(jnp.where(far_row[...] >= 0, 1.0, 0.0)).astype(jnp.int32)
    o = lax.shift_right_arithmetic(f, 6)
    s = jnp.where(live, f & 63, -1)
    oc = jnp.where(live, lax.shift_right_arithmetic(o, 5) * 4 + (o & 31) - (2 * j - 1), -1)
    a = (iota((16, 128), 0) == oc).astype(F32)
    oot[...] = a.astype(BF16)
    oo[...] = a.T.astype(BF16)
    a = (iota((64, 128), 0) == s).astype(F32)
    ost[...] = a.astype(BF16)
    os[...] = a.T.astype(BF16)
    f = far_row[...]
    live = f >= 0
    o = jnp.where(live, lax.shift_right_arithmetic(f, 6), -1)
    s = jnp.where(live, f & 63, -1)
    fot[...] = (iota((128, 384), 0) == o).astype(F32).astype(BF16)
    fst[...] = (iota((64, 384), 0) == s).astype(F32).astype(BF16)
    groups = lax.shift_right_logical(n + 7, 3)

    def leaving(g, part):
        at = pl.ds(8 * g + 4 * part, 4)
        return [
            pltpu.make_async_copy(built.at[g & 1, k, pl.ds(4 * part, 4)], out.at[at], out_sems.at[g & 1, k, part])
            for k, out in enumerate((kh, kl))
        ]

    def left_behind(g):
        for part in range(2):

            @pl.when(n > 8 * g + 4 * part)
            def _():
                for copy in leaving(g, part):
                    copy.wait()

    def eight(g, carry):
        @pl.when(g >= 2)
        def _():
            left_behind(g - 2)

        def one(b):
            t = 8 * g + b
            name = jnp.maximum(slots[0, t], 0)
            own = slice(8 * b, 8 * b + 8)
            for c in range(3):
                left[8 * b + c : 8 * b + c + 1, :] = points[c, pl.ds(lax.shift_right_logical(name, 6), 1), :]
                right[8 * b + c : 8 * b + c + 1, :] = sources[c, pl.ds(name & 63, 1), :]
            p, q = left[own, :], right[own, :]
            centre = 0.5 * (jnp.mean(p, axis=1, keepdims=True) + jnp.mean(q, axis=1, keepdims=True))
            p, q = p - centre, q - centre
            for c in range(3):
                pq[c, pl.ds(t, 1), :] = p[c : c + 1]
                pq[3 + c, pl.ds(t, 1), :] = q[c : c + 1]
            p1, p2, p3 = thirds(p)
            q1, q2, q3 = thirds(-2.0 * q)
            at = iota((8, 256), 0)
            end_p = jnp.where(at < 6, 1.0, 0.0)
            end_q = end_p
            for k, (x, y) in enumerate(
                zip(
                    thirds(jnp.sum(p * p, axis=0, keepdims=True)),
                    thirds(jnp.sum(q * q, axis=0, keepdims=True)),
                )
            ):
                end_p = jnp.where(at == k, x, end_p)
                end_q = jnp.where(at == k + 3, y, end_q)
            factor_p = jnp.concatenate([p1, p1, p2, p2, p1, p3, end_p, jnp.zeros((8, 256), F32)], axis=0)
            factor_q = jnp.concatenate([q1, q2, q1, q2, q3, q1, end_q, jnp.zeros((8, 256), F32)], axis=0)
            factor_q = factor_q.astype(BF16)
            factor_p = factor_p.astype(BF16).T
            for r in range(0, 256, 64):
                inverse = lax.rsqrt(mm(factor_p[r : r + 64], factor_q))
                square = inverse * inverse
                high, low = split(square * square * inverse)
                built[g & 1, 0, b, r : r + 64, :] = high
                built[g & 1, 1, b, r : r + 64, :] = low

        for b in range(4):
            one(b)
        for copy in leaving(g, 0):
            copy.start()

        @pl.when(n > 8 * g + 4)
        def _():
            for b in range(4, 8):
                one(b)
            for copy in leaving(g, 1):
                copy.start()

        return carry

    lax.fori_loop(0, groups, eight, 0)
    for back in (2, 1):

        @pl.when(groups >= back)
        def _():
            left_behind(groups - back)


def far_inputs(x, pick):
    high, low = split(x.T[0:64, :])
    return mm(high, pick) + mm(low, pick)


def far_outputs(terms, place):
    high, low = split(terms)
    return mm_nt(place, high) + mm_nt(place, low)


WIDE = 256


def far_copies(n, c, matrices, sem, act):
    @pl.when(n <= WIDE)
    def _():
        act(pltpu.make_async_copy(c.at[:, :, pl.ds(0, WIDE)], matrices.at[:, :, pl.ds(0, WIDE)], sem))

    @pl.when(n > WIDE)
    def _():
        act(pltpu.make_async_copy(c, matrices, sem))


def far_forward(n, x, pick, place, c, terms):
    v = far_inputs(x, pick)
    terms[...] = jnp.zeros_like(terms)

    def part(lanes):
        def eight(g, carry):
            rows = [jnp.sum(c[8 * g + b, :, lanes] * v[:, lanes], axis=0, keepdims=True) for b in range(8)]
            terms[pl.ds(pl.multiple_of(8 * g, 8), 8), lanes] = jnp.concatenate(rows, axis=0)
            return carry

        lax.fori_loop(0, 8, eight, 0)

    part(slice(0, WIDE))

    @pl.when(n > WIDE)
    def _():
        part(slice(WIDE, 320))

    return far_outputs(terms[...], place)


def far_adjoint(n, x, pick, place, c, terms, held):
    held[...] = far_inputs(x, pick)
    terms[...] = jnp.zeros_like(terms)

    def part(lanes):
        def eight(g, carry):
            rows = held[pl.ds(pl.multiple_of(8 * g, 8), 8), lanes.start : (lanes.stop + 127) // 128 * 128]
            for b in range(8):
                carry = carry + c[8 * g + b, :, lanes] * rows[b : b + 1, 0 : lanes.stop - lanes.start]
            return carry

        zeros = jnp.zeros((64, lanes.stop - lanes.start), F32)
        terms[0:64, lanes] = lax.fori_loop(0, 8, eight, zeros)

    part(slice(0, WIDE))

    @pl.when(n > WIDE)
    def _():
        part(slice(WIDE, 320))

    return far_outputs(terms[...], place)


def near_products(n, moments, results, kh, kl, forward, arrive=None):
    def four(first):
        for b in range(4):
            t = first + b
            at = pl.ds(pl.multiple_of(t * ROWS, ROWS), ROWS)
            high, low = split(jnp.concatenate([moments[0, at, :], moments[1, at, :]], axis=1))
            both = jnp.concatenate([high, low], axis=0)
            if forward:
                both = (mm_nt(kh[t], both) + mm_nt(kl[t], both)).T
            else:
                both = mm(both, kh[t]) + mm(both, kl[t])
            both = both[:ROWS] + both[ROWS:]
            results[0, at, :] = both[:, :128]
            results[1, at, :] = both[:, 128:]

    def eight(g, carry):
        if arrive is not None:
            arrive(g, 0)
            arrive(g, 1)
        four(8 * g)
        four(8 * g + 4)
        return carry

    whole = lax.shift_right_logical(n, 3)
    lax.fori_loop(0, whole, eight, 0)

    @pl.when((n & 7) > 0)
    def _():
        if arrive is not None:
            arrive(whole, 0)
        four(8 * whole)

        @pl.when((n & 7) > 4)
        def _():
            if arrive is not None:
                arrive(whole, 1)
            four(8 * whole + 4)


def store_moment(moments, g, c, value):
    at = pl.ds(g * (8 * ROWS) + c, 8, ROWS)
    moments.at[0][at, :] = value[:, :128]
    moments.at[1][at, :] = value[:, 128:]


def load_result(results, g, c):
    at = pl.ds(g * (8 * ROWS) + c, 8, ROWS)
    return jnp.concatenate([results.at[0][at, :], results.at[1][at, :]], axis=1)


def first_adjoint_block(
    count, column, recv, kh_far, kl_far, pq, oo, ost, fot, fst, c, out, kh, kl,
    yb, yp, moments, results, values, terms, held, matrices, sem, sems
):
    n = count[0]

    def arriving(g, part):
        at = pl.ds(8 * g + 4 * part, 4)
        return [
            pltpu.make_async_copy(a.at[at], b.at[at], sems.at[k, part, g])
            for k, (a, b) in enumerate(((kh_far, kh), (kl_far, kl)))
        ]

    def start(g, carry):
        for part in range(2):

            @pl.when(n > 8 * g + 4 * part)
            def _():
                for copy in arriving(g, part):
                    copy.start()

        return carry

    def arrive(g, part):
        for copy in arriving(g, part):
            copy.wait()

    far_copies(count[1], c, matrices, sem, lambda copy: copy.start())
    lax.fori_loop(0, lax.shift_right_logical(n + 7, 3), start, 0)
    adjoint_block(
        count, column, recv, kh, kl, pq, oo, ost, fot, fst, c, out,
        yb, yp, moments, results, values, terms, held, matrices, sem, arrive=arrive
    )


def adjoint_block(
    count, column, recv, kh, kl, pq, oo, ost, fot, fst, c, out,
    yb, yp, moments, results, values, terms, held, matrices, sem, arrive=None
):
    if arrive is None:
        far_copies(count[1], c, matrices, sem, lambda copy: copy.start())
    n = count[0]
    j = column[0]
    for t in range(4):
        col = 2 * j - 1 + t
        inside = jnp.logical_and(col >= 0, col < 32)
        holder = lax.shift_right_logical(jnp.clip(col, 0, 31), 3)
        for row in range(4):
            for half in range(2):
                piece = recv[row * 4 + holder, 2 * t + half : 2 * t + half + 1, 0:640]
                if t in (0, 3):
                    piece = jnp.where(inside, piece, 0.0)
                yb[4 * row + t : 4 * row + t + 1, 640 * half : 640 * half + 640] = piece
    high, low = split(yb[...])
    yp[...] = mm(oo[0:80, :], high) + mm(oo[0:80, :], low)
    values[...] = jnp.zeros_like(values)
    groups = lax.shift_right_logical(n + 7, 3)

    def enter(g, carry):
        at = pl.ds(pl.multiple_of(g * 8, 8), 8)
        hxx, hxy, hxz, hyy, hyz = (yp[at, 256 * a : 256 * a + 256] for a in range(5))
        hzz = -(hxx + hyy)
        px, py, pz = (pq[c, at, :] for c in range(3))
        ax, ay, az = hxx * px, hyy * py, hzz * pz
        bx, by, bz = hxy * py + hxz * pz, hxy * px + hyz * pz, hxz * px + hyz * py
        constant = px * (ax + hxy * py) + py * (ay + hyz * pz) + pz * (az + hxz * px)
        rows = (constant, 2.0 * ax + bx, 2.0 * ay + by, 2.0 * az + bz, hxx, hxy, hxz, hyy, hyz, hzz)
        for c, row in enumerate(rows):
            store_moment(moments, g, c, row)
        return carry

    lax.fori_loop(0, groups, enter, 0)
    tails = [recv[k, :, 640:768] for k in range(16)]

    def far():
        far_copies(count[1], c, matrices, sem, lambda copy: copy.wait())
        coeffs = far_adjoint(count[1], jnp.concatenate(tails, axis=0), fot[...], fst[...], matrices, terms, held)
        sums = functools.reduce(jnp.add, tails)
        for k in range(8):
            part = coeffs[8 * k : 8 * k + 8]
            out[8 * k : 8 * k + 8, 256:384] = jnp.where(iota((8, 128), 1) < 64, part, sums)

    if arrive is not None:
        far()
    near_products(n, moments, results, kh, kl, False, arrive)

    def leave(g, carry):
        at = pl.ds(pl.multiple_of(g * 8, 8), 8)
        w = [load_result(results, g, c) for c in range(10)]
        qx, qy, qz = (pq[3 + c, at, :] for c in range(3))
        z = w[0] + qx * (w[4] * qx + w[5] * qy - w[1]) + qy * (w[7] * qy + w[8] * qz - w[2])
        z = z + qz * (w[9] * qz + w[6] * qx - w[3])
        values[at, :] = jnp.where(iota((8, 256), 0) + g * 8 < n, z * (1.0 / 256.0), 0.0)
        return carry

    lax.fori_loop(0, groups, leave, 0)
    high, low = split(values[...])
    out[:, 0:256] = mm(ost[...], high) + mm(ost[...], low)
    if arrive is None:
        far()


def forward_block(
    count, column, recv, kh, kl, pq, os, oot, fot, fst, c, out,
    xp, moments, results, values, yb, terms, matrices, sem
):
    far_copies(count[1], c, matrices, sem, lambda copy: copy.start())
    n = count[0]
    j = column[0]
    high, low = split(recv[:, 0:256])
    xp[...] = mm(os[0:80, :], high) + mm(os[0:80, :], low)
    values[...] = jnp.zeros_like(values)
    groups = lax.shift_right_logical(n + 7, 3)

    def enter(g, carry):
        at = pl.ds(pl.multiple_of(g * 8, 8), 8)
        x = xp[at, :]
        qx, qy, qz = (pq[3 + c, at, :] for c in range(3))
        x1, x2, x3 = x * qx, x * qy, x * qz
        rows = (x, x1, x2, x3, x1 * qx, x1 * qy, x1 * qz, x2 * qy, x2 * qz, x3 * qz)
        for c, row in enumerate(rows):
            store_moment(moments, g, c, row)
        return carry

    lax.fori_loop(0, groups, enter, 0)
    near_products(n, moments, results, kh, kl, True)

    def leave(g, carry):
        at = pl.ds(pl.multiple_of(g * 8, 8), 8)
        s = [load_result(results, g, c) for c in range(10)]
        px, py, pz = (pq[c, at, :] for c in range(3))
        ax, ay, az = px * s[0] - s[1], py * s[0] - s[2], pz * s[0] - s[3]
        xx = px * (ax - s[1]) + s[4]
        xy = py * ax - px * s[2] + s[5]
        xz = pz * ax - px * s[3] + s[6]
        yy = py * (ay - s[2]) + s[7]
        yz = pz * ay - py * s[3] + s[8]
        zz = pz * (az - s[3]) + s[9]
        trace = xx + yy + zz
        inside = iota((8, 256), 0) + g * 8 < n
        parts = (3.0 * xx - trace, 3.0 * xy, 3.0 * xz, 3.0 * yy - trace, 3.0 * yz)
        for a, part in enumerate(parts):
            values[at, 256 * a : 256 * a + 256] = jnp.where(inside, part * (1.0 / 256.0), 0.0)
        return carry

    lax.fori_loop(0, groups, leave, 0)
    high, low = split(values[...])
    yb[...] = mm(oot[...], high) + mm(oot[...], low)
    for t in range(4):
        holder = lax.shift_right_logical(jnp.clip(2 * j - 1 + t, 0, 31), 3)
        for row in range(4):
            for half in range(2):
                piece = yb[4 * row + t : 4 * row + t + 1, 640 * half : 640 * half + 640]
                out[row * 4 + holder, 2 * t + half : 2 * t + half + 1, 0:640] = piece
    tails = [recv[8 * k : 8 * k + 8, 256:384] for k in range(8)]
    far_copies(count[1], c, matrices, sem, lambda copy: copy.wait())
    coeffs = far_forward(count[1], recv[:, 256:384], fst[...], fot[...], matrices, terms)
    sums = functools.reduce(jnp.add, tails)
    for k in range(16):
        out[k, :, 640:768] = jnp.where(iota((8, 128), 1) < 64, coeffs[8 * k : 8 * k + 8], sums)


def send_residual(zone, values, basis, out, weights, scalars, copies=()):
    y = [values[:, 256 * a : 256 * a + 256] for a in range(6)]
    trace = y[0] + y[3] + y[5]
    for a, part in enumerate((3.0 * y[0] - trace, 3.0 * y[1], 3.0 * y[2], 3.0 * y[3] - trace, 3.0 * y[4])):
        weights[:, 256 * a : 256 * a + 256] = part

    def rows(d):
        for t in range(4):
            r = 2 * d - 1 + t
            if 0 <= r < 8:
                for half in range(2):
                    piece = weights[r : r + 1, 640 * half : 640 * half + 640]
                    out[4 * zone + d, 2 * t + half : 2 * t + half + 1, 0:640] = piece

    for d in range(4):
        rows(d)

    @pl.when(zone > 0)
    def _():
        rows(-1)

    @pl.when(zone < 3)
    def _():
        rows(4)

    lanes = iota((64, 128), 1)
    columns = jnp.zeros((64, 128), F32)
    for r in range(8):
        if copies:
            copies[r].wait()
        column = jnp.sum(basis[r] * values[r : r + 1, :], axis=1, keepdims=True)
        columns = jnp.where(lanes == r, column, columns)
    columns = jnp.concatenate([columns, jnp.zeros((64, 128), F32)], axis=0)
    tail = with_scalars(columns.T[0:8, :], scalars)
    for k in range(16):
        out[k, :, 640:768] = tail


def start_obs(zone, data_far, basis_far, obs, src, out, points, sources, weights, data, basis, sem, sems):
    first = pltpu.make_async_copy(data_far, data, sem)
    first.start()
    copies = [pltpu.make_async_copy(basis_far.at[r], basis.at[r], sems.at[r]) for r in range(8)]
    for copy in copies:
        copy.start()
    others = [pltpu.make_async_copy(a, b, sems.at[k]) for k, a, b in ((8, obs, points), (9, src, sources))]
    for copy in others:
        copy.start()
    first.wait()
    send_residual(zone[0], data, basis, out, weights, (total(data[...] * data[...]),), copies)
    for copy in others:
        copy.wait()


def gather_projected(zone, recv, basis, near, p):
    tail = functools.reduce(jnp.add, [recv[k, :, 640:768] for k in range(16)])
    for r in range(8):
        for half in range(2):
            value = 0.0
            for t in range(4):
                if (r + 1 - t) % 2 == 0:
                    d = (r + 1 - t) // 2
                    piece = recv[jnp.clip(4 * zone + d, 0, 15), 2 * t + half : 2 * t + half + 1, 0:640]
                    if d == -1:
                        piece = jnp.where(zone > 0, piece, 0.0)
                    if d == 4:
                        piece = jnp.where(zone < 3, piece, 0.0)
                    value = value + piece
            near[r : r + 1, 640 * half : 640 * half + 640] = value
    columns = jnp.where(iota((8, 128), 1) < 64, tail, 0.0).T
    for r in range(8):
        p[r : r + 1, :] = jnp.sum(basis[r] * columns[0:64, r : r + 1], axis=0, keepdims=True)
    p[:, 0:1280] = p[:, 0:1280] + near[...]
    p[:, 1280:1536] = p[:, 1280:1536] - (near[:, 0:256] + near[:, 768:1024])
    return tail


def first_obs(zone, recv, data, basis, p, gammas, out, weights):
    z = zone[0]
    gammas[...] = gather_projected(z, recv, basis, weights, p)
    pv, dv = p[...], data[...]
    send_residual(z, p, basis, out, weights, (total(pv * pv), total(dv * pv)))


def second_obs(zone, recv, data, p0, gamma0, sums1, basis, p, r, gammas, out, weights):
    z = zone[0]
    tail = gather_projected(z, recv, basis, weights, p)
    gammas[...] = tail
    g0 = lane_scalar(gamma0[...], 0)
    pv = p[...] + (lane_scalar(tail, 0) / g0) * p0[...]
    rv = data[...] - (g0 / lane_scalar(sums1[...], 0)) * p0[...]
    p[...] = pv
    r[...] = rv
    send_residual(z, p, basis, out, weights, (total(pv * pv), total(rv * pv)))


def gather_normal(recv, basis, q):
    block = functools.reduce(jnp.add, [recv[k] for k in range(8)])
    tail = block[:, 256:384]
    columns = jnp.where(iota((8, 128), 1) < 64, tail, 0.0).T
    for r in range(8):
        far = jnp.sum(basis[r] * columns[0:64, r : r + 1], axis=0, keepdims=True)
        q[r : r + 1, :] = block[r : r + 1, 0:256] + far
    return tail


def send_direction(x, basis, out):
    lanes = iota((64, 128), 1)
    columns = jnp.zeros((64, 128), F32)
    for r in range(8):
        column = jnp.sum(basis[r] * x[r : r + 1], axis=1, keepdims=True)
        columns = jnp.where(lanes == r, column, columns)
    columns = jnp.concatenate([columns, jnp.zeros((64, 128), F32)], axis=0)
    tail = with_scalars(columns.T[0:8, :], (total(x * x),))
    for k in range(8):
        out[k, :, 0:256] = x
        out[k, :, 256:384] = tail


def first_src(recv, basis, n0, sums, out):
    sums[...] = gather_normal(recv, basis, n0)
    send_direction(n0[...], basis, out)


def second_src(recv, basis, n0, gamma0, n1, sums, out):
    tail = gather_normal(recv, basis, n1)
    sums[...] = tail
    x = n0[...] - (lane_scalar(gamma0[...], 0) / lane_scalar(tail, 0)) * n1[...]
    n1[...] = x
    send_direction(x, basis, out)


def last_src(recv, basis, n0, n1, gamma0, gamma1, sums0, sums1, r1, p1, found, residual, normal, misfit):
    tail = gather_normal(recv, basis, normal)
    g0, g1 = lane_scalar(gamma0[...], 0), lane_scalar(gamma1[...], 0)
    s1 = sums1[...]
    curve0, cross0 = lane_scalar(s1, 0), lane_scalar(s1, 1)
    curve1, cross1 = lane_scalar(tail, 0), lane_scalar(tail, 1)
    step0, step1 = g0 / curve0, g1 / curve1
    normal[...] = n1[...] - step1 * normal[...]
    found[...] = step0 * n0[...] + step1 * (n1[...] + (g1 / g0) * n0[...])
    residual[...] = r1[...] - step1 * p1[...]
    m0 = lane_scalar(sums0[...], 0)
    m1 = m0 - 2.0 * step0 * cross0 + step0 * step0 * curve0
    m2 = m1 - 2.0 * step1 * cross1 + step1 * step1 * curve1
    for k, value in enumerate((m0, m1, m2)):
        misfit[k] = value[0, 0]


VM = pl.BlockSpec(memory_space=pltpu.VMEM)
SM = pl.BlockSpec(memory_space=pltpu.SMEM)
FAR = pl.BlockSpec(memory_space=pltpu.HBM)


def shape(*dims, dtype=F32):
    return jax.ShapeDtypeStruct(dims, dtype)


def call(kernel, outs, ins, scratch=(), out_specs=None, scalars=0, far=(), limit=4):
    specs = [SM] * scalars + [VM] * (len(ins) - scalars)
    for at in far:
        specs[at] = FAR
    ins = [pltpu.with_memory_space_constraint(a, pltpu.HBM) if k in far else a for k, a in enumerate(ins)]
    return pl.pallas_call(
        kernel,
        out_shape=outs,
        in_specs=specs,
        out_specs=out_specs or [VM] * len(outs),
        scratch_shapes=list(scratch),
        compiler_params=pltpu.CompilerParams(vmem_limit_bytes=limit * MIB),
    )(*ins)


def exchange(value, axes):
    return lax.all_to_all(value, axes, split_axis=0, concat_axis=0, tiled=True)


def shards(data, obs_points, src_points, obs_basis, src_basis, couplings, near_pairs, far_pairs):
    index = lax.axis_index(SRC).astype(jnp.int32)
    column = index.reshape(1)
    zone = (index % 4).reshape(1)
    obs_message = shape(16, 8, 768)
    src_message = shape(8, 8, 384)
    row = shape(8, 128)
    dma = pltpu.SemaphoreType.DMA

    def bf(*dims):
        return shape(*dims, dtype=BF16)

    message, points, sources = call(
        start_obs,
        [obs_message, shape(3, 128, 256), shape(3, 64, 256)],
        [
            zone, data, obs_basis,
            jnp.transpose(obs_points, (1, 0, 2)), jnp.transpose(src_points, (1, 0, 2)),
        ],
        scalars=1,
        far=(1, 2, 3, 4),
        scratch=[pltpu.VMEM((8, 1280), F32), pltpu.VMEM((8, 1536), F32), pltpu.VMEM((8, 64, 1536), F32), dma, dma((10,))],
        limit=LIMIT0,
    )
    received = exchange(message, SRC)
    kh_far, kl_far, pq, count, oo, oot, ost, os, fot, fst = call(
        setup_near,
        [
            *[pltpu.HBM((PAIRS, 256, 256), BF16)] * 2, shape(6, PAIRS, 256), shape(2, dtype=jnp.int32),
            bf(128, 16), bf(16, 128), bf(64, 128), bf(128, 64), bf(128, 384), bf(64, 384),
        ],
        [
            column, near_pairs.reshape(1, 72), far_pairs.reshape(1, 320), points, sources,
        ],
        scalars=1,
        far=(1, 2),
        out_specs=[FAR] * 2 + [VM] + [SM] + [VM] * 6,
        scratch=[
            pltpu.SMEM((1, 72), jnp.int32), pltpu.VMEM((1, 72), jnp.int32), pltpu.VMEM((1, 320), jnp.int32),
            pltpu.VMEM((1, 128), jnp.int32), pltpu.VMEM((1, 384), jnp.int32), pltpu.VMEM((64, 256), F32), pltpu.VMEM((64, 256), F32),
            pltpu.VMEM((2, 2, 8, 256, 256), BF16), dma((3,)), dma((2, 2, 2)),
        ],
        limit=LIMIT0,
    )
    matrices = jnp.transpose(couplings[0, 0], (1, 2, 0))
    matrix_scratch = [pltpu.VMEM((64, 64, 320), F32), dma]
    adjoint_scratch = [
        pltpu.VMEM((16, 1280), F32), pltpu.VMEM((80, 1280), F32), pltpu.VMEM((2, 80 * ROWS, 128), F32),
        pltpu.VMEM((2, 80 * ROWS, 128), F32), pltpu.VMEM((128, 256), F32), pltpu.VMEM((128, 384), F32),
        pltpu.VMEM((64, 384), F32), *matrix_scratch,
    ]
    out, kh, kl = call(
        first_adjoint_block,
        [shape(64, 384), bf(PAIRS, 256, 256), bf(PAIRS, 256, 256)],
        [count, column, received, kh_far, kl_far, pq, oo, ost, fot, fst, matrices],
        scalars=2,
        far=(3, 4, 10),
        scratch=[*adjoint_scratch, dma((2, 2, 9))],
        limit=LIMIT,
    )
    received = exchange(out.reshape(8, 8, 384), OBS)

    def adjoint(message):
        (out,) = call(
            adjoint_block,
            [shape(64, 384)],
            [count, column, message, kh, kl, pq, oo, ost, fot, fst, matrices],
            scalars=2,
            far=(10,),
            scratch=adjoint_scratch,
            limit=LIMIT,
        )
        return exchange(out.reshape(8, 8, 384), OBS)

    def forward(message):
        (out,) = call(
            forward_block,
            [obs_message],
            [count, column, exchange(message, OBS).reshape(64, 384), kh, kl, pq, os, oot, fot, fst, matrices],
            scalars=2,
            far=(10,),
            scratch=[
                pltpu.VMEM((80, 256), F32), pltpu.VMEM((2, 80 * ROWS, 128), F32), pltpu.VMEM((2, 80 * ROWS, 128), F32),
                pltpu.VMEM((128, 1280), F32), pltpu.VMEM((16, 1280), F32), pltpu.VMEM((128, 384), F32),
                *matrix_scratch,
            ],
            limit=LIMIT,
        )
        return exchange(out, SRC)

    plane, line = shape(8, 1536), shape(8, 256)
    n0, sums0, message = call(first_src, [line, row, src_message], [received, src_basis])
    p0, gamma0, message = call(
        first_obs, [plane, row, obs_message], [zone, forward(message), data, obs_basis], scalars=1,
        scratch=[pltpu.VMEM((8, 1280), F32)],
    )
    n1, sums1, message = call(
        second_src, [line, row, src_message], [adjoint(exchange(message, SRC)), src_basis, n0, gamma0]
    )
    p1, r1, gamma1, message = call(
        second_obs,
        [plane, plane, row, obs_message],
        [zone, forward(message), data, p0, gamma0, sums1, obs_basis],
        scalars=1,
        scratch=[pltpu.VMEM((8, 1280), F32)],
    )
    found, residual, normal, misfit = call(
        last_src,
        [line, plane, line, shape(3)],
        [adjoint(exchange(message, SRC)), src_basis, n0, n1, gamma0, gamma1, sums0, sums1, r1, p1],
        out_specs=[VM] * 3 + [SM],
    )
    return found, residual, normal, misfit


def solution(mesh):
    finer = Mesh(mesh.devices.reshape(4, 2, 4, 4), ("obs_0", "obs_1", "src_0", "src_1"))
    return jax.shard_map(
        shards,
        mesh=finer,
        in_specs=(
            P(OBS_SRC, None),
            P(OBS, None, None),
            P(SRC, None, None),
            P(OBS_SRC, None, None),
            P(SRC_OBS, None, None),
            P(OBS, SRC, None, None, None),
            P(OBS, SRC, None),
            P(OBS, SRC, None),
        ),
        out_specs=(P(SRC_OBS, None), P(OBS_SRC, None), P(SRC_OBS, None), P()),
        check_vma=False,
    )
```

```python
import functools

import jax
import jax.numpy as jnp
from jax import lax
from jax.experimental import pallas as pl
from jax.experimental.pallas import tpu as pltpu
from jax.sharding import Mesh
from jax.sharding import PartitionSpec as P

OBS_SRC = ("obs_0", "obs_1", "src_0", "src_1")
SRC = ("src_0", "src_1")
OBS = ("obs_0", "obs_1")
SRC_OBS = ("src_0", "src_1", "obs_0", "obs_1")

F32 = jnp.float32
BF16 = jnp.bfloat16
PAIRS = 72
ROWS = 16
MIB = 1 << 20
LIMIT0 = 8
LIMIT = 10


def split(value):
    high = value.astype(BF16)
    return high, (value - high.astype(F32)).astype(BF16)


def thirds(value):
    first = value.astype(BF16).astype(F32)
    rest = value - first
    second = rest.astype(BF16).astype(F32)
    return first, second, (rest - second).astype(BF16).astype(F32)


def mm(a, b):
    return lax.dot_general(a, b, (((1,), (0,)), ((), ())), preferred_element_type=F32)


def mm_nt(a, b):
    return lax.dot_general(a, b, (((1,), (1,)), ((), ())), preferred_element_type=F32)


def iota(shape, dim):
    return lax.broadcasted_iota(jnp.int32, shape, dim)


def lane_scalar(block, which):
    lanes = iota(block.shape, 1)
    return jnp.sum(jnp.where(lanes == 64 + which, block, 0.0), axis=1, keepdims=True)


def total(value):
    return jnp.sum(jnp.sum(value, axis=1, keepdims=True), axis=0, keepdims=True)


def with_scalars(block, scalars):
    lanes = iota(block.shape, 1)
    for which, value in enumerate(scalars):
        block = jnp.where(lanes == 64 + which, value, block)
    return block


def setup_near(
    column, near, far, points, sources, kh, kl, pq, count, oo, oot, ost, os, fot, fst,
    slots, near_part, far_part, near_row, far_row, left, right, built, sems, out_sems
):
    copies = [
        pltpu.make_async_copy(a, b, sems.at[k])
        for k, (a, b) in enumerate(
            ((near, slots), (near, near_part), (far, far_part))
        )
    ]
    for copy in copies:
        copy.start()
    j = column[0]
    near_row[...] = jnp.full_like(near_row, -1)
    far_row[...] = jnp.full_like(far_row, -1)
    left[...] = jnp.zeros_like(left)
    right[...] = jnp.zeros_like(right)
    for copy in copies:
        copy.wait()
    near_row[:, 0:72] = near_part[...]
    far_row[:, 0:320] = far_part[...]
    f = near_row[...]
    live = f >= 0
    n = jnp.sum(jnp.where(live, 1.0, 0.0)).astype(jnp.int32)
    count[0] = n
    count[1] = jnp.sum(jnp.where(far_row[...] >= 0, 1.0, 0.0)).astype(jnp.int32)
    o = lax.shift_right_arithmetic(f, 6)
    s = jnp.where(live, f & 63, -1)
    oc = jnp.where(live, lax.shift_right_arithmetic(o, 5) * 4 + (o & 31) - (2 * j - 1), -1)
    a = (iota((16, 128), 0) == oc).astype(F32)
    oot[...] = a.astype(BF16)
    oo[...] = a.T.astype(BF16)
    a = (iota((64, 128), 0) == s).astype(F32)
    ost[...] = a.astype(BF16)
    os[...] = a.T.astype(BF16)
    f = far_row[...]
    live = f >= 0
    o = jnp.where(live, lax.shift_right_arithmetic(f, 6), -1)
    s = jnp.where(live, f & 63, -1)
    fot[...] = (iota((128, 384), 0) == o).astype(F32).astype(BF16)
    fst[...] = (iota((64, 384), 0) == s).astype(F32).astype(BF16)
    groups = lax.shift_right_logical(n + 7, 3)

    def leaving(g, part):
        at = pl.ds(8 * g + 4 * part, 4)
        return [
            pltpu.make_async_copy(built.at[g & 1, k, pl.ds(4 * part, 4)], out.at[at], out_sems.at[g & 1, k, part])
            for k, out in enumerate((kh, kl))
        ]

    def left_behind(g):
        for part in range(2):

            @pl.when(n > 8 * g + 4 * part)
            def _():
                for copy in leaving(g, part):
                    copy.wait()

    def eight(g, carry):
        @pl.when(g >= 2)
        def _():
            left_behind(g - 2)

        def one(b):
            t = 8 * g + b
            name = jnp.maximum(slots[0, t], 0)
            own = slice(8 * b, 8 * b + 8)
            for c in range(3):
                left[8 * b + c : 8 * b + c + 1, :] = points[c, pl.ds(lax.shift_right_logical(name, 6), 1), :]
                right[8 * b + c : 8 * b + c + 1, :] = sources[c, pl.ds(name & 63, 1), :]
            p, q = left[own, :], right[own, :]
            centre = 0.5 * (jnp.mean(p, axis=1, keepdims=True) + jnp.mean(q, axis=1, keepdims=True))
            p, q = p - centre, q - centre
            for c in range(3):
                pq[c, pl.ds(t, 1), :] = p[c : c + 1]
                pq[3 + c, pl.ds(t, 1), :] = q[c : c + 1]
            p1, p2, p3 = thirds(p)
            q1, q2, q3 = thirds(-2.0 * q)
            at = iota((8, 256), 0)
            end_p = jnp.where(at < 6, 1.0, 0.0)
            end_q = end_p
            for k, (x, y) in enumerate(
                zip(
                    thirds(jnp.sum(p * p, axis=0, keepdims=True)),
                    thirds(jnp.sum(q * q, axis=0, keepdims=True)),
                )
            ):
                end_p = jnp.where(at == k, x, end_p)
                end_q = jnp.where(at == k + 3, y, end_q)
            factor_p = jnp.concatenate([p1, p1, p2, p2, p1, p3, end_p, jnp.zeros((8, 256), F32)], axis=0)
            factor_q = jnp.concatenate([q1, q2, q1, q2, q3, q1, end_q, jnp.zeros((8, 256), F32)], axis=0)
            factor_q = factor_q.astype(BF16)
            factor_p = factor_p.astype(BF16).T
            for r in range(0, 256, 64):
                inverse = lax.rsqrt(mm(factor_p[r : r + 64], factor_q))
                square = inverse * inverse
                high, low = split(square * square * inverse)
                built[g & 1, 0, b, r : r + 64, :] = high
                built[g & 1, 1, b, r : r + 64, :] = low

        for b in range(4):
            one(b)
        for copy in leaving(g, 0):
            copy.start()

        @pl.when(n > 8 * g + 4)
        def _():
            for b in range(4, 8):
                one(b)
            for copy in leaving(g, 1):
                copy.start()

        return carry

    lax.fori_loop(0, groups, eight, 0)
    for back in (2, 1):

        @pl.when(groups >= back)
        def _():
            left_behind(groups - back)


def far_inputs(x, pick):
    high, low = split(x.T[0:64, :])
    return mm(high, pick) + mm(low, pick)


def far_outputs(terms, place):
    high, low = split(terms)
    return mm_nt(place, high) + mm_nt(place, low)


WIDE = 256


def far_copies(n, c, matrices, sem, act):
    @pl.when(n <= WIDE)
    def _():
        act(pltpu.make_async_copy(c.at[:, :, pl.ds(0, WIDE)], matrices.at[:, :, pl.ds(0, WIDE)], sem))

    @pl.when(n > WIDE)
    def _():
        act(pltpu.make_async_copy(c, matrices, sem))


def far_forward_group(g, c, lanes, terms, held):
    v = held[:, lanes]
    rows = [jnp.sum(c[8 * g + b, :, lanes] * v, axis=0, keepdims=True) for b in range(8)]
    terms[pl.ds(pl.multiple_of(8 * g, 8), 8), lanes] = jnp.concatenate(rows, axis=0)


def far_adjoint_group(g, c, lanes, terms, held):
    rows = held[pl.ds(pl.multiple_of(8 * g, 8), 8), lanes.start : (lanes.stop + 127) // 128 * 128]
    value = terms[0:64, lanes]
    for b in range(8):
        value = value + c[8 * g + b, :, lanes] * rows[b : b + 1, 0 : lanes.stop - lanes.start]
    terms[0:64, lanes] = value


def far_rest(first, n, group, c, terms, held):
    def some(lanes, first):
        def one(g, carry):
            group(g, c, lanes, terms, held)
            return carry

        lax.fori_loop(first, 8, one, 0)

    some(slice(0, WIDE), first)

    @pl.when(n > WIDE)
    def _():
        some(slice(WIDE, 320), 0)


def near_products(n, moments, results, kh, kl, forward, arrive=None, beside=None):
    def four(first):
        for b in range(4):
            t = first + b
            at = pl.ds(pl.multiple_of(t * ROWS, ROWS), ROWS)
            high, low = split(jnp.concatenate([moments[0, at, :], moments[1, at, :]], axis=1))
            both = jnp.concatenate([high, low], axis=0)
            if forward:
                both = mm_nt(both, kh[t]) + mm_nt(both, kl[t])
            else:
                both = mm(both, kh[t]) + mm(both, kl[t])
            both = both[:ROWS] + both[ROWS:]
            results[0, at, :] = both[:, :128]
            results[1, at, :] = both[:, 128:]

    def eight(g, carry):
        if arrive is not None:
            arrive(g, 0)
            arrive(g, 1)
        four(8 * g)
        if beside is not None:
            beside(g)
        four(8 * g + 4)
        return carry

    whole = lax.shift_right_logical(n, 3)
    lax.fori_loop(0, jnp.minimum(whole, 8), eight, 0)

    @pl.when(whole == 9)
    def _():
        if arrive is not None:
            arrive(8, 0)
            arrive(8, 1)
        four(64)
        four(68)

    @pl.when((n & 7) > 0)
    def _():
        if arrive is not None:
            arrive(whole, 0)
        four(8 * whole)

        @pl.when((n & 7) > 4)
        def _():
            if arrive is not None:
                arrive(whole, 1)
            four(8 * whole + 4)


def store_moment(moments, g, c, value):
    at = pl.ds(g * (8 * ROWS) + c, 8, ROWS)
    moments.at[0][at, :] = value[:, :128]
    moments.at[1][at, :] = value[:, 128:]


def load_result(results, g, c):
    at = pl.ds(g * (8 * ROWS) + c, 8, ROWS)
    return jnp.concatenate([results.at[0][at, :], results.at[1][at, :]], axis=1)


def first_adjoint_block(
    count, column, recv, kh_far, kl_far, pq, oo, ost, fot, fst, matrices, out, kh, kl, c,
    yb, yp, moments, results, values, terms, held, sem, sems
):
    n = count[0]

    def arriving(g, part):
        at = pl.ds(8 * g + 4 * part, 4)
        return [
            pltpu.make_async_copy(a.at[at], b.at[at], sems.at[k, part, g])
            for k, (a, b) in enumerate(((kh_far, kh), (kl_far, kl)))
        ]

    def start(g, carry):
        for part in range(2):

            @pl.when(n > 8 * g + 4 * part)
            def _():
                for copy in arriving(g, part):
                    copy.start()

        return carry

    def arrive(g, part):
        for copy in arriving(g, part):
            copy.wait()

    far_copies(count[1], matrices, c, sem, lambda copy: copy.start())
    lax.fori_loop(0, lax.shift_right_logical(n + 7, 3), start, 0)
    adjoint_block(
        count, column, recv, kh, kl, pq, oo, ost, fot, fst, c, out,
        yb, yp, moments, results, values, terms, held, matrices, sem, arrive
    )


def adjoint_block(
    count, column, recv, kh, kl, pq, oo, ost, fot, fst, c, out,
    yb, yp, moments, results, values, terms, held, matrices=None, sem=None, arrive=None
):
    n = count[0]
    j = column[0]
    for t in range(4):
        col = 2 * j - 1 + t
        inside = jnp.logical_and(col >= 0, col < 32)
        holder = lax.shift_right_logical(jnp.clip(col, 0, 31), 3)
        for row in range(4):
            for half in range(2):
                piece = recv[row * 4 + holder, 2 * t + half : 2 * t + half + 1, 0:640]
                if t in (0, 3):
                    piece = jnp.where(inside, piece, 0.0)
                yb[4 * row + t : 4 * row + t + 1, 640 * half : 640 * half + 640] = piece
    high, low = split(yb[...])
    yp[...] = mm(oo[0:80, :], high) + mm(oo[0:80, :], low)
    values[...] = jnp.zeros_like(values)
    groups = lax.shift_right_logical(n + 7, 3)

    def enter(g, carry):
        at = pl.ds(pl.multiple_of(g * 8, 8), 8)
        hxx, hxy, hxz, hyy, hyz = (yp[at, 256 * a : 256 * a + 256] for a in range(5))
        hzz = -(hxx + hyy)
        px, py, pz = (pq[c, at, :] for c in range(3))
        ax, ay, az = hxx * px, hyy * py, hzz * pz
        bx, by, bz = hxy * py + hxz * pz, hxy * px + hyz * pz, hxz * px + hyz * py
        constant = px * (ax + hxy * py) + py * (ay + hyz * pz) + pz * (az + hxz * px)
        rows = (constant, 2.0 * ax + bx, 2.0 * ay + by, 2.0 * az + bz, hxx, hxy, hxz, hyy, hyz, hzz)
        for c, row in enumerate(rows):
            store_moment(moments, g, c, row)
        return carry

    lax.fori_loop(0, groups, enter, 0)
    tails = [recv[k, :, 640:768] for k in range(16)]
    held[...] = far_inputs(jnp.concatenate(tails, axis=0), fot[...])
    terms[...] = jnp.zeros_like(terms)

    def beside(g):
        far_adjoint_group(g, c, slice(0, WIDE), terms, held)

    if arrive is None:
        near_products(n, moments, results, kh, kl, False, None, beside)
        far_rest(lax.shift_right_logical(n, 3), count[1], far_adjoint_group, c, terms, held)
    else:
        far_copies(count[1], matrices, c, sem, lambda copy: copy.wait())
        far_rest(0, count[1], far_adjoint_group, c, terms, held)
        near_products(n, moments, results, kh, kl, False, arrive)
    coeffs = far_outputs(terms[...], fst[...])
    sums = functools.reduce(jnp.add, tails)
    for k in range(8):
        part = coeffs[8 * k : 8 * k + 8]
        out[8 * k : 8 * k + 8, 256:384] = jnp.where(iota((8, 128), 1) < 64, part, sums)

    def leave(g, carry):
        at = pl.ds(pl.multiple_of(g * 8, 8), 8)
        w = [load_result(results, g, c) for c in range(10)]
        qx, qy, qz = (pq[3 + c, at, :] for c in range(3))
        z = w[0] + qx * (w[4] * qx + w[5] * qy - w[1]) + qy * (w[7] * qy + w[8] * qz - w[2])
        z = z + qz * (w[9] * qz + w[6] * qx - w[3])
        values[at, :] = jnp.where(iota((8, 256), 0) + g * 8 < n, z * (1.0 / 256.0), 0.0)
        return carry

    lax.fori_loop(0, groups, leave, 0)
    high, low = split(values[...])
    out[:, 0:256] = mm(ost[:, 0:80], high) + mm(ost[:, 0:80], low)


def forward_block(
    count, column, recv, kh, kl, pq, os, oot, fot, fst, c, out,
    xp, moments, results, values, yb, terms, held
):
    n = count[0]
    j = column[0]
    high, low = split(recv[:, 0:256])
    xp[...] = mm(os[0:80, :], high) + mm(os[0:80, :], low)
    values[...] = jnp.zeros_like(values)
    groups = lax.shift_right_logical(n + 7, 3)

    def enter(g, carry):
        at = pl.ds(pl.multiple_of(g * 8, 8), 8)
        x = xp[at, :]
        qx, qy, qz = (pq[3 + c, at, :] for c in range(3))
        x1, x2, x3 = x * qx, x * qy, x * qz
        rows = (x, x1, x2, x3, x1 * qx, x1 * qy, x1 * qz, x2 * qy, x2 * qz, x3 * qz)
        for c, row in enumerate(rows):
            store_moment(moments, g, c, row)
        return carry

    lax.fori_loop(0, groups, enter, 0)
    held[...] = far_inputs(recv[:, 256:384], fst[...])
    terms[...] = jnp.zeros_like(terms)
    near_products(
        n, moments, results, kh, kl, True, None,
        lambda g: far_forward_group(g, c, slice(0, WIDE), terms, held),
    )
    far_rest(lax.shift_right_logical(n, 3), count[1], far_forward_group, c, terms, held)

    def leave(g, carry):
        at = pl.ds(pl.multiple_of(g * 8, 8), 8)
        s = [load_result(results, g, c) for c in range(10)]
        px, py, pz = (pq[c, at, :] for c in range(3))
        ax, ay, az = px * s[0] - s[1], py * s[0] - s[2], pz * s[0] - s[3]
        xx = px * (ax - s[1]) + s[4]
        xy = py * ax - px * s[2] + s[5]
        xz = pz * ax - px * s[3] + s[6]
        yy = py * (ay - s[2]) + s[7]
        yz = pz * ay - py * s[3] + s[8]
        zz = pz * (az - s[3]) + s[9]
        trace = xx + yy + zz
        inside = iota((8, 256), 0) + g * 8 < n
        parts = (3.0 * xx - trace, 3.0 * xy, 3.0 * xz, 3.0 * yy - trace, 3.0 * yz)
        for a, part in enumerate(parts):
            values[at, 256 * a : 256 * a + 256] = jnp.where(inside, part * (1.0 / 256.0), 0.0)
        return carry

    lax.fori_loop(0, groups, leave, 0)
    high, low = split(values[...])
    yb[...] = mm(oot[:, 0:80], high) + mm(oot[:, 0:80], low)
    for t in range(4):
        holder = lax.shift_right_logical(jnp.clip(2 * j - 1 + t, 0, 31), 3)
        for row in range(4):
            for half in range(2):
                piece = yb[4 * row + t : 4 * row + t + 1, 640 * half : 640 * half + 640]
                out[row * 4 + holder, 2 * t + half : 2 * t + half + 1, 0:640] = piece
    tails = [recv[8 * k : 8 * k + 8, 256:384] for k in range(8)]
    coeffs = far_outputs(terms[...], fot[...])
    sums = functools.reduce(jnp.add, tails)
    for k in range(16):
        out[k, :, 640:768] = jnp.where(iota((8, 128), 1) < 64, coeffs[8 * k : 8 * k + 8], sums)


def send_residual(zone, values, basis, out, weights, scalars, copies=()):
    y = [values[:, 256 * a : 256 * a + 256] for a in range(6)]
    trace = y[0] + y[3] + y[5]
    for a, part in enumerate((3.0 * y[0] - trace, 3.0 * y[1], 3.0 * y[2], 3.0 * y[3] - trace, 3.0 * y[4])):
        weights[:, 256 * a : 256 * a + 256] = part

    def rows(d):
        for t in range(4):
            r = 2 * d - 1 + t
            if 0 <= r < 8:
                for half in range(2):
                    piece = weights[r : r + 1, 640 * half : 640 * half + 640]
                    out[4 * zone + d, 2 * t + half : 2 * t + half + 1, 0:640] = piece

    for d in range(4):
        rows(d)

    @pl.when(zone > 0)
    def _():
        rows(-1)

    @pl.when(zone < 3)
    def _():
        rows(4)

    lanes = iota((64, 128), 1)
    columns = jnp.zeros((64, 128), F32)
    for r in range(8):
        if copies:
            copies[r].wait()
        column = jnp.sum(basis[r] * values[r : r + 1, :], axis=1, keepdims=True)
        columns = jnp.where(lanes == r, column, columns)
    columns = jnp.concatenate([columns, jnp.zeros((64, 128), F32)], axis=0)
    tail = with_scalars(columns.T[0:8, :], scalars)
    for k in range(16):
        out[k, :, 640:768] = tail


def start_obs(zone, data_far, basis_far, obs, src, out, points, sources, weights, data, basis, sem, sems):
    first = pltpu.make_async_copy(data_far, data, sem)
    first.start()
    copies = [pltpu.make_async_copy(basis_far.at[r], basis.at[r], sems.at[r]) for r in range(8)]
    for copy in copies:
        copy.start()
    others = [pltpu.make_async_copy(a, b, sems.at[k]) for k, a, b in ((8, obs, points), (9, src, sources))]
    for copy in others:
        copy.start()
    first.wait()
    send_residual(zone[0], data, basis, out, weights, (total(data[...] * data[...]),), copies)
    for copy in others:
        copy.wait()


def gather_projected(zone, recv, basis, near, p):
    tail = functools.reduce(jnp.add, [recv[k, :, 640:768] for k in range(16)])
    for r in range(8):
        for half in range(2):
            value = 0.0
            for t in range(4):
                if (r + 1 - t) % 2 == 0:
                    d = (r + 1 - t) // 2
                    piece = recv[jnp.clip(4 * zone + d, 0, 15), 2 * t + half : 2 * t + half + 1, 0:640]
                    if d == -1:
                        piece = jnp.where(zone > 0, piece, 0.0)
                    if d == 4:
                        piece = jnp.where(zone < 3, piece, 0.0)
                    value = value + piece
            near[r : r + 1, 640 * half : 640 * half + 640] = value
    columns = jnp.where(iota((8, 128), 1) < 64, tail, 0.0).T
    for r in range(8):
        p[r : r + 1, :] = jnp.sum(basis[r] * columns[0:64, r : r + 1], axis=0, keepdims=True)
    p[:, 0:1280] = p[:, 0:1280] + near[...]
    p[:, 1280:1536] = p[:, 1280:1536] - (near[:, 0:256] + near[:, 768:1024])
    return tail


def first_obs(zone, recv, data, basis, p, gammas, out, weights):
    z = zone[0]
    gammas[...] = gather_projected(z, recv, basis, weights, p)
    pv, dv = p[...], data[...]
    send_residual(z, p, basis, out, weights, (total(pv * pv), total(dv * pv)))


def second_obs(zone, recv, data, p0, gamma0, sums1, basis, p, r, gammas, out, weights):
    z = zone[0]
    tail = gather_projected(z, recv, basis, weights, p)
    gammas[...] = tail
    g0 = lane_scalar(gamma0[...], 0)
    pv = p[...] + (lane_scalar(tail, 0) / g0) * p0[...]
    rv = data[...] - (g0 / lane_scalar(sums1[...], 0)) * p0[...]
    p[...] = pv
    r[...] = rv
    send_residual(z, p, basis, out, weights, (total(pv * pv), total(rv * pv)))


def gather_normal(recv, basis, q):
    block = functools.reduce(jnp.add, [recv[k] for k in range(8)])
    tail = block[:, 256:384]
    columns = jnp.where(iota((8, 128), 1) < 64, tail, 0.0).T
    for r in range(8):
        far = jnp.sum(basis[r] * columns[0:64, r : r + 1], axis=0, keepdims=True)
        q[r : r + 1, :] = block[r : r + 1, 0:256] + far
    return tail


def send_direction(x, basis, out):
    lanes = iota((64, 128), 1)
    columns = jnp.zeros((64, 128), F32)
    for r in range(8):
        column = jnp.sum(basis[r] * x[r : r + 1], axis=1, keepdims=True)
        columns = jnp.where(lanes == r, column, columns)
    columns = jnp.concatenate([columns, jnp.zeros((64, 128), F32)], axis=0)
    tail = with_scalars(columns.T[0:8, :], (total(x * x),))
    for k in range(8):
        out[k, :, 0:256] = x
        out[k, :, 256:384] = tail


def first_src(recv, basis, n0, sums, out):
    sums[...] = gather_normal(recv, basis, n0)
    send_direction(n0[...], basis, out)


def second_src(recv, basis, n0, gamma0, n1, sums, out):
    tail = gather_normal(recv, basis, n1)
    sums[...] = tail
    x = n0[...] - (lane_scalar(gamma0[...], 0) / lane_scalar(tail, 0)) * n1[...]
    n1[...] = x
    send_direction(x, basis, out)


def last_src(recv, basis, n0, n1, gamma0, gamma1, sums0, sums1, r1, p1, found, residual, normal, misfit):
    tail = gather_normal(recv, basis, normal)
    g0, g1 = lane_scalar(gamma0[...], 0), lane_scalar(gamma1[...], 0)
    s1 = sums1[...]
    curve0, cross0 = lane_scalar(s1, 0), lane_scalar(s1, 1)
    curve1, cross1 = lane_scalar(tail, 0), lane_scalar(tail, 1)
    step0, step1 = g0 / curve0, g1 / curve1
    normal[...] = n1[...] - step1 * normal[...]
    found[...] = step0 * n0[...] + step1 * (n1[...] + (g1 / g0) * n0[...])
    residual[...] = r1[...] - step1 * p1[...]
    m0 = lane_scalar(sums0[...], 0)
    m1 = m0 - 2.0 * step0 * cross0 + step0 * step0 * curve0
    m2 = m1 - 2.0 * step1 * cross1 + step1 * step1 * curve1
    for k, value in enumerate((m0, m1, m2)):
        misfit[k] = value[0, 0]


VM = pl.BlockSpec(memory_space=pltpu.VMEM)
SM = pl.BlockSpec(memory_space=pltpu.SMEM)
FAR = pl.BlockSpec(memory_space=pltpu.HBM)


def shape(*dims, dtype=F32):
    return jax.ShapeDtypeStruct(dims, dtype)


def call(kernel, outs, ins, scratch=(), out_specs=None, scalars=0, far=(), limit=4):
    specs = [SM] * scalars + [VM] * (len(ins) - scalars)
    for at in far:
        specs[at] = FAR
    ins = [pltpu.with_memory_space_constraint(a, pltpu.HBM) if k in far else a for k, a in enumerate(ins)]
    return pl.pallas_call(
        kernel,
        out_shape=outs,
        in_specs=specs,
        out_specs=out_specs or [VM] * len(outs),
        scratch_shapes=list(scratch),
        compiler_params=pltpu.CompilerParams(vmem_limit_bytes=limit * MIB),
    )(*ins)


def exchange(value, axes):
    return lax.all_to_all(value, axes, split_axis=0, concat_axis=0, tiled=True)


def shards(data, obs_points, src_points, obs_basis, src_basis, couplings, near_pairs, far_pairs):
    index = lax.axis_index(SRC).astype(jnp.int32)
    column = index.reshape(1)
    zone = (index % 4).reshape(1)
    obs_message = shape(16, 8, 768)
    src_message = shape(8, 8, 384)
    row = shape(8, 128)
    dma = pltpu.SemaphoreType.DMA

    def bf(*dims):
        return shape(*dims, dtype=BF16)

    message, points, sources = call(
        start_obs,
        [obs_message, shape(3, 128, 256), shape(3, 64, 256)],
        [
            zone, data, obs_basis,
            jnp.transpose(obs_points, (1, 0, 2)), jnp.transpose(src_points, (1, 0, 2)),
        ],
        scalars=1,
        far=(1, 2, 3, 4),
        scratch=[pltpu.VMEM((8, 1280), F32), pltpu.VMEM((8, 1536), F32), pltpu.VMEM((8, 64, 1536), F32), dma, dma((10,))],
        limit=LIMIT0,
    )
    received = exchange(message, SRC)
    kh_far, kl_far, pq, count, oo, oot, ost, os, fot, fst = call(
        setup_near,
        [
            *[pltpu.HBM((PAIRS, 256, 256), BF16)] * 2, shape(6, PAIRS, 256), shape(2, dtype=jnp.int32),
            bf(128, 16), bf(16, 128), bf(64, 128), bf(128, 64), bf(128, 384), bf(64, 384),
        ],
        [
            column, near_pairs.reshape(1, 72), far_pairs.reshape(1, 320), points, sources,
        ],
        scalars=1,
        far=(1, 2),
        out_specs=[FAR] * 2 + [VM] + [SM] + [VM] * 6,
        scratch=[
            pltpu.SMEM((1, 72), jnp.int32), pltpu.VMEM((1, 72), jnp.int32), pltpu.VMEM((1, 320), jnp.int32),
            pltpu.VMEM((1, 128), jnp.int32), pltpu.VMEM((1, 384), jnp.int32), pltpu.VMEM((64, 256), F32), pltpu.VMEM((64, 256), F32),
            pltpu.VMEM((2, 2, 8, 256, 256), BF16), dma((3,)), dma((2, 2, 2)),
        ],
        limit=LIMIT0,
    )
    matrices = jnp.transpose(couplings[0, 0], (1, 2, 0))
    adjoint_scratch = [
        pltpu.VMEM((16, 1280), F32), pltpu.VMEM((80, 1280), F32), pltpu.VMEM((2, 80 * ROWS, 128), F32),
        pltpu.VMEM((2, 80 * ROWS, 128), F32), pltpu.VMEM((80, 256), F32), pltpu.VMEM((128, 384), F32),
        pltpu.VMEM((64, 384), F32),
    ]
    out, kh, kl, held = call(
        first_adjoint_block,
        [shape(64, 384), bf(PAIRS, 256, 256), bf(PAIRS, 256, 256), shape(64, 64, 320)],
        [count, column, received, kh_far, kl_far, pq, oo, ost, fot, fst, matrices],
        scalars=2,
        far=(3, 4, 10),
        scratch=[*adjoint_scratch, dma, dma((2, 2, 9))],
        limit=LIMIT,
    )
    received = exchange(out.reshape(8, 8, 384), OBS)

    def adjoint(message):
        (out,) = call(
            adjoint_block,
            [shape(64, 384)],
            [count, column, message, kh, kl, pq, oo, ost, fot, fst, held],
            scalars=2,
            scratch=adjoint_scratch,
            limit=LIMIT,
        )
        return exchange(out.reshape(8, 8, 384), OBS)

    def forward(message):
        (out,) = call(
            forward_block,
            [obs_message],
            [count, column, exchange(message, OBS).reshape(64, 384), kh, kl, pq, os, oot, fot, fst, held],
            scalars=2,
            scratch=[
                pltpu.VMEM((80, 256), F32), pltpu.VMEM((2, 80 * ROWS, 128), F32), pltpu.VMEM((2, 80 * ROWS, 128), F32),
                pltpu.VMEM((80, 1280), F32), pltpu.VMEM((16, 1280), F32), pltpu.VMEM((128, 384), F32),
                pltpu.VMEM((64, 384), F32),
            ],
            limit=LIMIT,
        )
        return exchange(out, SRC)

    plane, line = shape(8, 1536), shape(8, 256)
    n0, sums0, message = call(first_src, [line, row, src_message], [received, src_basis])
    p0, gamma0, message = call(
        first_obs, [plane, row, obs_message], [zone, forward(message), data, obs_basis], scalars=1,
        scratch=[pltpu.VMEM((8, 1280), F32)],
    )
    n1, sums1, message = call(
        second_src, [line, row, src_message], [adjoint(exchange(message, SRC)), src_basis, n0, gamma0]
    )
    p1, r1, gamma1, message = call(
        second_obs,
        [plane, plane, row, obs_message],
        [zone, forward(message), data, p0, gamma0, sums1, obs_basis],
        scalars=1,
        scratch=[pltpu.VMEM((8, 1280), F32)],
    )
    found, residual, normal, misfit = call(
        last_src,
        [line, plane, line, shape(3)],
        [adjoint(exchange(message, SRC)), src_basis, n0, n1, gamma0, gamma1, sums0, sums1, r1, p1],
        out_specs=[VM] * 3 + [SM],
    )
    return found, residual, normal, misfit


def solution(mesh):
    finer = Mesh(mesh.devices.reshape(4, 2, 4, 4), ("obs_0", "obs_1", "src_0", "src_1"))
    return jax.shard_map(
        shards,
        mesh=finer,
        in_specs=(
            P(OBS_SRC, None),
            P(OBS, None, None),
            P(SRC, None, None),
            P(OBS_SRC, None, None),
            P(SRC_OBS, None, None),
            P(OBS, SRC, None, None, None),
            P(OBS, SRC, None),
            P(OBS, SRC, None),
        ),
        out_specs=(P(SRC_OBS, None), P(OBS_SRC, None), P(SRC_OBS, None), P()),
        check_vma=False,
    )
```
